256 devices in a mesh: dp: 32 (over z, y), fsdp: 8 (over x, core).
Axes of the slice: x: 4, y: 4, z: 8, core: 2. Of those that a mesh axis runs over, the one named last changes fastest.
Arguments:
- dec_in: bfloat16 [512, 384, 512], P(('dp', 'fsdp'))
- enc_out: bfloat16 [512, 384, 512], P(('dp', 'fsdp'))
- src_lens: int32 [512], P(('dp', 'fsdp'))
- tgt_lens: int32 [512], P(('dp', 'fsdp'))
- y_cot: bfloat16 [512, 384, 512], P(('dp', 'fsdp'))
- attn_w: bfloat16 [4096, 512], P('fsdp')
- ffn_w: bfloat16 [4096, 512], P('fsdp')
- vec_params: bfloat16 [9728], P('fsdp')
Outputs:
- output 1: bfloat16 [512, 384, 512], P(('dp', 'fsdp'))
- output 2: bfloat16 [512, 384, 512], P(('dp', 'fsdp'))
- output 3: bfloat16 [512, 384, 512], P(('dp', 'fsdp'))
- output 4: float32 [4096, 512], P('fsdp')
- output 5: float32 [4096, 512], P('fsdp')
- output 6: float32 [9728], P('fsdp')
All inputs are finite; a program needn't handle non-finite values.
Results may differ from the reference program's by a relative error of at most 0.0165577.
Values are sent between devices in bfloat16 or wider.
A program may use at most 768 MiB of HBM per device.

```python
import jax
import jax.numpy as jnp
from jax import lax

BATCH_ALL = 512
TGT_LEN = 384
SRC_LEN = 384
D_MODEL = 512
NUM_HEADS = 8
FFN_DIM = 2048
HEAD_DIM = D_MODEL // NUM_HEADS
VEC_LEN = 15 * D_MODEL + FFN_DIM


def setup_inputs(seed: int = 0) -> dict:
    key_list = jax.random.split(jax.random.key(seed), 10)
    token_shift = 0.5 * jax.random.normal(key_list[0], (BATCH_ALL, TGT_LEN, 1), jnp.float32)
    column_mean = 0.3 * jax.random.normal(key_list[1], (1, 1, D_MODEL), jnp.float32)
    x_val = jax.random.normal(key_list[2], (BATCH_ALL, TGT_LEN, D_MODEL), jnp.float32) + token_shift + column_mean
    enc_val = jax.random.normal(key_list[3], (BATCH_ALL, SRC_LEN, D_MODEL), jnp.float32)
    src_draw = jax.random.randint(key_list[4], (BATCH_ALL,), SRC_LEN // 4, SRC_LEN + 1)
    tgt_draw = jax.random.randint(key_list[5], (BATCH_ALL,), TGT_LEN // 4, TGT_LEN + 1)
    first_row = jnp.arange(BATCH_ALL) == 0
    src_lens = jnp.where(first_row, SRC_LEN, src_draw).astype(jnp.int32)
    tgt_lens = jnp.where(first_row, TGT_LEN, tgt_draw).astype(jnp.int32)
    dy_val = jax.random.normal(key_list[6], (BATCH_ALL, TGT_LEN, D_MODEL), jnp.float32)
    attn_val = jax.random.normal(key_list[7], (8 * D_MODEL, D_MODEL), jnp.float32) * D_MODEL ** -0.5
    row_ids = jnp.arange(2 * FFN_DIM)[:, None]
    ffn_scale = jnp.where(row_ids < FFN_DIM, D_MODEL ** -0.5, FFN_DIM ** -0.5)
    ffn_val = jax.random.normal(key_list[8], (2 * FFN_DIM, D_MODEL), jnp.float32) * ffn_scale
    slot_ids = jnp.arange(VEC_LEN) // D_MODEL
    is_gain = ((slot_ids == 9) | (slot_ids == 11) | (slot_ids == 13)).astype(jnp.float32)
    vec_val = 0.3 * jax.random.normal(key_list[9], (VEC_LEN,), jnp.float32) + is_gain
    return {'dec_in': x_val.astype(jnp.bfloat16), 'enc_out': enc_val.astype(jnp.bfloat16), 'src_lens': src_lens, 'tgt_lens': tgt_lens, 'y_cot': dy_val.astype(jnp.bfloat16), 'attn_w': attn_val.astype(jnp.bfloat16), 'ffn_w': ffn_val.astype(jnp.bfloat16), 'vec_params': vec_val.astype(jnp.bfloat16)}


def layer_norm(resid_in, vec_f, slot_idx):
    ln_gain = vec_f[slot_idx * D_MODEL:(slot_idx + 1) * D_MODEL]
    ln_shift = vec_f[(slot_idx + 1) * D_MODEL:(slot_idx + 2) * D_MODEL]
    row_mean = jnp.mean(resid_in, axis=-1, keepdims=True)
    centred = resid_in - row_mean
    row_var = jnp.mean(centred * centred, axis=-1, keepdims=True)
    return centred * lax.rsqrt(row_var + 1e-5) * ln_gain + ln_shift


def attend(q_rows, k_rows, v_rows, key_mask):
    q_heads = q_rows.astype(jnp.float32).reshape(q_rows.shape[0], NUM_HEADS, HEAD_DIM)
    k_heads = k_rows.astype(jnp.float32).reshape(k_rows.shape[0], NUM_HEADS, HEAD_DIM)
    v_heads = v_rows.astype(jnp.float32).reshape(v_rows.shape[0], NUM_HEADS, HEAD_DIM)
    scores = jnp.einsum('qhd,khd->hqk', q_heads, k_heads)
    scores = jnp.where(key_mask[None], scores, -1e30)
    attn_prob = jax.nn.softmax(scores, axis=-1).astype(jnp.bfloat16).astype(jnp.float32)
    attn_out = jnp.einsum('hqk,khd->qhd', attn_prob, v_heads)
    return attn_out.reshape(q_rows.shape[0], D_MODEL).astype(jnp.bfloat16)


def layer_one(x_row, enc_row, src_n, tgt_n, attn_f, ffn_f, vec_f):
    def linear(h_rows, slot_idx):
        w_mat = attn_f[slot_idx * D_MODEL:(slot_idx + 1) * D_MODEL]
        b_vec = vec_f[slot_idx * D_MODEL:(slot_idx + 1) * D_MODEL]
        return jnp.dot(h_rows, w_mat, preferred_element_type=jnp.float32) + b_vec

    x_f = x_row.astype(jnp.float32)
    enc_f = enc_row.astype(jnp.float32)
    tgt_pos = jnp.arange(TGT_LEN)
    self_mask = (tgt_pos[None, :] <= tgt_pos[:, None]) & (tgt_pos[None, :] < tgt_n)
    cross_mask = jnp.broadcast_to(jnp.arange(SRC_LEN)[None, :] < src_n, (TGT_LEN, SRC_LEN))
    q_self = (linear(x_f, 0) * 0.125).astype(jnp.bfloat16)
    k_self = linear(x_f, 1).astype(jnp.bfloat16)
    v_self = linear(x_f, 2).astype(jnp.bfloat16)
    o_self = attend(q_self, k_self, v_self, self_mask).astype(jnp.float32)
    h_one = layer_norm(x_f + linear(o_self, 3), vec_f, 9).astype(jnp.bfloat16).astype(jnp.float32)
    q_cross = (linear(h_one, 4) * 0.125).astype(jnp.bfloat16)
    k_cross = linear(enc_f, 5).astype(jnp.bfloat16)
    v_cross = linear(enc_f, 6).astype(jnp.bfloat16)
    o_cross = attend(q_cross, k_cross, v_cross, cross_mask).astype(jnp.float32)
    h_two = layer_norm(h_one + linear(o_cross, 7), vec_f, 11).astype(jnp.bfloat16).astype(jnp.float32)
    up_proj = jnp.dot(h_two, ffn_f[:FFN_DIM].T, preferred_element_type=jnp.float32) + vec_f[15 * D_MODEL:]
    gelu_out = jax.nn.gelu(up_proj, approximate=False).astype(jnp.bfloat16).astype(jnp.float32)
    down_proj = jnp.dot(gelu_out, ffn_f[FFN_DIM:], preferred_element_type=jnp.float32) + vec_f[8 * D_MODEL:9 * D_MODEL]
    return layer_norm(h_two + down_proj, vec_f, 13).astype(jnp.bfloat16)


def reference(dec_in, enc_out, src_lens, tgt_lens, y_cot, attn_w, ffn_w, vec_params):
    attn_f = attn_w.astype(jnp.float32)
    ffn_f = ffn_w.astype(jnp.float32)
    vec_f = vec_params.astype(jnp.float32)

    def one_sample(grad_sums, sample):
        x_row, enc_row, src_n, tgt_n, cot_row = sample

        def forward(x_arg, enc_arg, attn_arg, ffn_arg, vec_arg):
            return layer_one(x_arg, enc_arg, src_n, tgt_n, attn_arg, ffn_arg, vec_arg)

        y_row, pull_back = jax.vjp(forward, x_row, enc_row, attn_f, ffn_f, vec_f)
        dx_row, denc_row, g_attn, g_ffn, g_vec = pull_back(cot_row)
        new_sums = (grad_sums[0] + g_attn, grad_sums[1] + g_ffn, grad_sums[2] + g_vec)
        return new_sums, (y_row, dx_row, denc_row)

    zero_sums = (jnp.zeros_like(attn_f), jnp.zeros_like(ffn_f), jnp.zeros_like(vec_f))
    grad_sums, outs_stack = lax.scan(one_sample, zero_sums, (dec_in, enc_out, src_lens, tgt_lens, y_cot))
    grad_scale = 1.0 / (BATCH_ALL * TGT_LEN)
    return outs_stack[0], outs_stack[1], outs_stack[2], grad_sums[0] * grad_scale, grad_sums[1] * grad_scale, grad_sums[2] * grad_scale
```

```python
import functools
import jax
import jax.numpy as jnp
from jax import lax
from jax.experimental import pallas as pl
from jax.experimental.pallas import tpu as pltpu
from jax.sharding import PartitionSpec as P

LN_EPS = 1e-5
MASK_FILL = -1e30
BF = jnp.bfloat16
F32 = jnp.float32
ROWS = 256


def mm(a, b):
    return lax.dot_general(a, b, (((1,), (0,)), ((), ())), preferred_element_type=F32)


def mm_nt(a, b):
    return lax.dot_general(a, b, (((1,), (1,)), ((), ())), preferred_element_type=F32)


def mm_tn(a, b):
    return lax.dot_general(a, b, (((0,), (0,)), ((), ())), preferred_element_type=F32)


def layer_kernel(n_batch, n_tgt, n_src, d_model, ffn_dim, src_lens, tgt_lens, x, enc, dy, aw, fw, vec, y, dx, denc, ga, gf, gv,
                 q, k, v, o, h1, n1, i1, qc, kc, vc, oc, n2, i2, h2, gp, g, acc, dres, dresb):
    n_ffn = ffn_dim // d_model
    n_tok = n_batch * n_tgt
    n_chunks = n_tok // ROWS
    n_pairs = d_model // 128

    def rows(r):
        return pl.ds(pl.multiple_of(r * ROWS, ROWS), ROWS)

    def bias(i):
        return vec[i:i + 1, :]

    def add_vec(i, val):
        gv[pl.ds(i, 1), :] += jnp.sum(val, axis=0, keepdims=True)

    def norm(res):
        cen = res - jnp.mean(res, axis=-1, keepdims=True)
        inv = lax.rsqrt(jnp.mean(cen * cen, axis=-1, keepdims=True) + LN_EPS)
        return cen * inv, inv

    def norm_grad(d_out, normed, inv, slot):
        add_vec(slot, d_out * normed)
        add_vec(slot + 1, d_out)
        d_norm = d_out * bias(slot)
        return inv * (d_norm - jnp.mean(d_norm, axis=-1, keepdims=True) - normed * jnp.mean(d_norm * normed, axis=-1, keepdims=True))

    gv[...] = jnp.zeros_like(gv)

    def proj_self(r, _):
        s = rows(r)
        xr = x[s, :]
        er = enc[s, :]
        q[s, :] = ((mm(xr, aw[0]) + bias(0)) * 0.125).astype(BF)
        k[s, :] = (mm(xr, aw[1]) + bias(1)).astype(BF)
        v[s, :] = (mm(xr, aw[2]) + bias(2)).astype(BF)
        kc[s, :] = (mm(er, aw[5]) + bias(5)).astype(BF)
        vc[s, :] = (mm(er, aw[6]) + bias(6)).astype(BF)
        return 0

    lax.fori_loop(0, n_chunks, proj_self, 0)

    low_half = lax.broadcasted_iota(jnp.int32, (n_tgt, 128), 1) < 64

    def half(val, j):
        return jnp.where(low_half if j == 0 else ~low_half, val, jnp.zeros_like(val))

    def key_mask(b, causal):
        key_pos = lax.broadcasted_iota(jnp.int32, (n_tgt, n_src), 1)
        if causal:
            return (key_pos <= lax.broadcasted_iota(jnp.int32, (n_tgt, n_src), 0)) & (key_pos < tgt_lens[b])
        return key_pos < src_lens[b]

    def prob(qm, k2, mask):
        sc = jnp.where(mask, mm_nt(qm, k2), MASK_FILL)
        e = jnp.exp(sc - jnp.max(sc, axis=-1, keepdims=True))
        return e * (1.0 / jnp.sum(e, axis=-1, keepdims=True))

    def attn(q, k, v, o, causal):
        def step(i, _):
            b = i // n_pairs
            hp = i % n_pairs
            s = pl.ds(pl.multiple_of(b * n_tgt, n_tgt), n_tgt)
            c = pl.ds(pl.multiple_of(hp * 128, 128), 128)
            q2, k2, v2 = q[s, c], k[s, c], v[s, c]
            mask = key_mask(b, causal)
            outs = [mm(prob(half(q2, j), k2, mask).astype(BF), v2) for j in range(2)]
            o[s, c] = jnp.where(low_half, outs[0], outs[1]).astype(BF)
            return 0
        lax.fori_loop(0, n_batch * n_pairs, step, 0)

    def attn_grad(q, k, v, do, causal):
        def step(i, _):
            b = i // n_pairs
            hp = i % n_pairs
            s = pl.ds(pl.multiple_of(b * n_tgt, n_tgt), n_tgt)
            c = pl.ds(pl.multiple_of(hp * 128, 128), 128)
            q2, k2, v2, do2 = q[s, c], k[s, c], v[s, c], do[s, c]
            mask = key_mask(b, causal)
            qt, dot = q2.T, do2.T
            dq, dkt, dvt = [], [], []
            for j in range(2):
                p = prob(half(q2, j), k2, mask)
                dp = mm_nt(half(do2, j), v2)
                dvt.append(mm(dot[64 * j:64 * j + 64], p.astype(BF)))
                ds = (p * (dp - jnp.sum(p * dp, axis=-1, keepdims=True))).astype(BF)
                dq.append(mm(ds, k2))
                dkt.append(mm(qt[64 * j:64 * j + 64], ds))
            q[s, c] = (jnp.where(low_half, dq[0], dq[1]) * 0.125).astype(BF)
            k[s, c] = jnp.concatenate(dkt, axis=0).astype(BF).T
            v[s, c] = jnp.concatenate(dvt, axis=0).astype(BF).T
            return 0
        lax.fori_loop(0, n_batch * n_pairs, step, 0)

    attn(q, k, v, o, True)

    def post_self(r, _):
        s = rows(r)
        n1[s, :], i1[s, :] = norm(x[s, :].astype(F32) + mm(o[s, :], aw[3]) + bias(3))
        h = (n1[s, :] * bias(9) + bias(10)).astype(BF)
        h1[s, :] = h
        qc[s, :] = ((mm(h, aw[4]) + bias(4)) * 0.125).astype(BF)
        return 0

    lax.fori_loop(0, n_chunks, post_self, 0)
    attn(qc, kc, vc, oc, False)

    def ffn(r, _):
        s = rows(r)
        n2[s, :], i2[s, :] = norm(h1[s, :].astype(F32) + mm(oc[s, :], aw[7]) + bias(7))
        h = (n2[s, :] * bias(11) + bias(12)).astype(BF)
        h2[s, :] = h
        acc[s, :] = h.astype(F32) + bias(8)

        def up(f, _):
            u = mm_nt(h2[s, :], fw[f]) + vec[pl.ds(15 + f, 1), :]
            cdf = 0.5 * (1.0 + lax.erf(u * 0.7071067811865476))
            g_out = (u * cdf).astype(BF)
            g[f, s, :] = g_out
            gp[f, s, :] = cdf + u * (0.3989422804014327 * jnp.exp(-0.5 * u * u))
            acc[s, :] += mm(g_out, fw[n_ffn + f])
            return 0

        lax.fori_loop(0, n_ffn, up, 0)
        normed, inv = norm(acc[s, :])
        y[s, :] = (normed * bias(13) + bias(14)).astype(BF)
        d3 = norm_grad(dy[s, :].astype(F32), normed, inv, 13)
        add_vec(8, d3)
        dres[s, :] = d3
        dresb[s, :] = d3.astype(BF)
        return 0

    lax.fori_loop(0, n_chunks, ffn, 0)

    def ffn_grad(f, _):
        gf[n_ffn + f] = mm_tn(g[f], dresb[...])

        def up_grad(r, _):
            s = rows(r)
            d_up = mm_nt(dresb[s, :], fw[n_ffn + f]) * gp[f, s, :]
            add_vec(15 + f, d_up)
            d_up = d_up.astype(BF)
            g[f, s, :] = d_up
            dres[s, :] += mm(d_up, fw[f])
            return 0

        lax.fori_loop(0, n_chunks, up_grad, 0)
        gf[f] = mm_tn(g[f], h2[...])
        return 0

    lax.fori_loop(0, n_ffn, ffn_grad, 0)

    def norm2_grad(r, _):
        s = rows(r)
        d2 = norm_grad(dres[s, :], n2[s, :], i2[s, :], 11)
        add_vec(7, d2)
        dres[s, :] = d2
        d2 = d2.astype(BF)
        dresb[s, :] = d2
        h2[s, :] = mm_nt(d2, aw[7]).astype(BF)
        return 0

    lax.fori_loop(0, n_chunks, norm2_grad, 0)
    ga[7] = mm_tn(oc[...], dresb[...])
    attn_grad(qc, kc, vc, h2, False)
    ga[4] = mm_tn(h1[...], qc[...])
    ga[5] = mm_tn(enc[...], kc[...])
    ga[6] = mm_tn(enc[...], vc[...])

    def norm1_grad(r, _):
        s = rows(r)
        add_vec(4, qc[s, :].astype(F32))
        add_vec(5, kc[s, :].astype(F32))
        add_vec(6, vc[s, :].astype(F32))
        denc[s, :] = (mm_nt(kc[s, :], aw[5]) + mm_nt(vc[s, :], aw[6])).astype(BF)
        d1 = norm_grad(dres[s, :] + mm_nt(qc[s, :], aw[4]), n1[s, :], i1[s, :], 9)
        add_vec(3, d1)
        dres[s, :] = d1
        d1 = d1.astype(BF)
        dresb[s, :] = d1
        h2[s, :] = mm_nt(d1, aw[3]).astype(BF)
        return 0

    lax.fori_loop(0, n_chunks, norm1_grad, 0)
    ga[3] = mm_tn(o[...], dresb[...])
    attn_grad(q, k, v, h2, True)
    ga[0] = mm_tn(x[...], q[...])
    ga[1] = mm_tn(x[...], k[...])
    ga[2] = mm_tn(x[...], v[...])

    def last(r, _):
        s = rows(r)
        add_vec(0, q[s, :].astype(F32))
        add_vec(1, k[s, :].astype(F32))
        add_vec(2, v[s, :].astype(F32))
        dx[s, :] = (dres[s, :] + mm_nt(q[s, :], aw[0]) + mm_nt(k[s, :], aw[1]) + mm_nt(v[s, :], aw[2])).astype(BF)
        return 0

    lax.fori_loop(0, n_chunks, last, 0)


def local_layer(dec_in, enc_out, src_lens, tgt_lens, y_cot, aw, fw, vec):
    n_batch, n_tgt, d = dec_in.shape
    n_src = enc_out.shape[1]
    n_tok = n_batch * n_tgt
    ffn_dim = fw.shape[0] * d // 2
    tok = lambda dt: pltpu.VMEM((n_tok, d), dt)
    n_ffn = ffn_dim // d
    vm = pl.BlockSpec(memory_space=pltpu.VMEM)
    sm = pl.BlockSpec(memory_space=pltpu.SMEM)
    act = jax.ShapeDtypeStruct((n_tok, d), BF)
    col = pltpu.VMEM((n_tok, 1), F32)
    y, dx, denc, ga, gf, gv = pl.pallas_call(
        functools.partial(layer_kernel, n_batch, n_tgt, n_src, d, ffn_dim),
        out_shape=(act, act, act, jax.ShapeDtypeStruct(aw.shape, F32), jax.ShapeDtypeStruct(fw.shape, F32), jax.ShapeDtypeStruct(vec.shape, F32)),
        in_specs=[sm, sm] + [vm] * 6,
        out_specs=(vm,) * 6,
        scratch_shapes=[tok(BF)] * 4 + [tok(BF), tok(F32), col] + [tok(BF)] * 4 + [tok(F32), col, tok(BF),
                        pltpu.VMEM((n_ffn, n_tok, d), F32), pltpu.VMEM((n_ffn, n_tok, d), BF), tok(F32), tok(F32), tok(BF)],
        compiler_params=pltpu.CompilerParams(vmem_limit_bytes=67043328),
        cost_estimate=pl.CostEstimate(flops=24 * 10**9, bytes_accessed=30 * 2**20, transcendentals=0),
        name='layer',
    )(src_lens, tgt_lens, dec_in.reshape(n_tok, d), enc_out.reshape(n_tok, d), y_cot.reshape(n_tok, d), aw, fw, vec)
    return y.reshape(dec_in.shape), dx.reshape(dec_in.shape), denc.reshape(enc_out.shape), ga, gf, gv


def solution(mesh):
    n_fsdp = mesh.shape['fsdp']
    n_dp = mesh.shape['dp']
    batch_axes = ('dp', 'fsdp')
    act_spec = P(batch_axes, None, None)
    len_spec = P(batch_axes)
    row_spec = P('fsdp', None)
    vec_spec = P('fsdp')

    def device_step(dec_in, enc_out, src_lens, tgt_lens, y_cot, attn_w, ffn_w, vec_params):
        d = attn_w.shape[1]
        n_vec = vec_params.shape[0]
        vec_rows = -(-n_vec // d)
        vec_pad = jnp.pad(vec_params, (0, vec_rows * d - n_vec)).reshape(vec_rows, d)
        packed = lax.all_gather(jnp.concatenate([attn_w, vec_pad], axis=0), 'fsdp', axis=0)
        aw = packed[:, :d]
        vec = packed[:, d:].reshape(n_fsdp, vec_rows * d)[:, :n_vec].reshape(-1, d).astype(F32)
        fw = lax.all_gather(ffn_w, 'fsdp', axis=0)
        y, dx, denc, ga, gf, gv = local_layer(dec_in, enc_out, src_lens, tgt_lens, y_cot, aw, fw, vec)
        scale = 1.0 / (dec_in.shape[0] * dec_in.shape[1] * n_fsdp * n_dp)
        gv = lax.psum(gv.reshape(n_fsdp, n_vec), batch_axes)
        gv = lax.dynamic_index_in_dim(gv, lax.axis_index('fsdp'), 0, keepdims=False)
        ga = lax.psum_scatter(ga.reshape(-1, d), 'fsdp', scatter_dimension=0, tiled=True)
        gf = lax.psum_scatter(gf.reshape(-1, d), 'fsdp', scatter_dimension=0, tiled=True)
        ga, gf = lax.psum((ga, gf), 'dp')
        return y, dx, denc, ga * scale, gf * scale, gv * scale

    return jax.shard_map(device_step, mesh=mesh, in_specs=(act_spec, act_spec, len_spec, len_spec, act_spec, row_spec, row_spec, vec_spec), out_specs=(act_spec, act_spec, act_spec, row_spec, row_spec, vec_spec), check_vma=False)
```

```python
import functools
import jax
import jax.numpy as jnp
from jax import lax
from jax.experimental import pallas as pl
from jax.experimental.pallas import tpu as pltpu
from jax.sharding import PartitionSpec as P

LN_EPS = 1e-5
MASK_FILL = -1e30
BF = jnp.bfloat16
F32 = jnp.float32
ROWS = 256


def mm(a, b):
    return lax.dot_general(a, b, (((1,), (0,)), ((), ())), preferred_element_type=F32)


def mm_nt(a, b):
    return lax.dot_general(a, b, (((1,), (1,)), ((), ())), preferred_element_type=F32)


def mm_tn(a, b):
    return lax.dot_general(a, b, (((0,), (0,)), ((), ())), preferred_element_type=F32)


N_X = 4
N_Y = 4
N_Z = 8
MESH = pl.DeviceIdType.MESH


def layer_kernel(n_batch, n_tgt, n_src, d_model, ffn_dim, scale, src_lens, tgt_lens, x, enc, dy, attn_w, ffn_w, vec_w,
                 y, dx, denc, attn_out, ffn_out, vec_out,
                 aw, fw, ga, gf, gv, vec, vec_all, q, k, v, o, h1, n1, i1, qc, kc, vc, oc, n2, i2, h2, gp, g, dres, dresb,
                 a1, a2, b1, b2, c1, c2, e1, e2, z_in, vec_pair, vec_x, vec_y, vec_z, send_sems, recv_sems):
    acc = dres
    n_ffn = ffn_dim // d_model
    n_tok = n_batch * n_tgt
    n_chunks = n_tok // ROWS
    n_pairs = d_model // 128
    half_rows = d_model // 2
    y_rows = half_rows // N_Y
    z_rows = y_rows // N_Z

    dp = lax.axis_index('dp')
    fs = lax.axis_index('fsdp')
    my_z, my_y = dp // N_Y, dp % N_Y
    my_x, core = fs // 2, fs % 2
    other = 1 - core
    sem_count = [0]

    def along_x(step):
        return (dp, (my_x + step) % N_X * 2 + core)

    def along_y(step):
        return (my_z * N_Y + (my_y + step) % N_Y, fs)

    def along_z(step):
        return ((my_z + step) % N_Z * N_Y + my_y, fs)

    partner = (dp, my_x * 2 + other)

    def new_sem():
        sem_count[0] += 1
        return sem_count[0] - 1

    def remote(src, dst, sem, device):
        return pltpu.make_async_remote_copy(src_ref=src, dst_ref=dst, send_sem=send_sems.at[sem], recv_sem=recv_sems.at[sem], device_id=device, device_id_type=MESH)

    def send(src, dst, device):
        copy = remote(src, dst, new_sem(), device)
        copy.start()
        return copy

    barrier = pltpu.get_barrier_semaphore()
    peers = [(dp, (fs + i) % (2 * N_X)) for i in range(1, 2 * N_X)]
    peers += [along_y(i) for i in range(1, N_Y)] + [along_z(i) for i in range(1, N_Z)]
    for peer in peers:
        pl.semaphore_signal(barrier, inc=1, device_id=peer, device_id_type=MESH)
    pl.semaphore_wait(barrier, len(peers))

    class Gather:
        def __init__(self, block, full):
            self.block, self.full, self.copies = block, full, []
            self.xs = [(my_x + i) % N_X for i in range(N_X)]

        def go(self, src, device):
            self.copies.append(send(src, src, device))
            return self.copies[-1]

        def start(self):
            mine = self.full.at[fs]
            self.up = send(self.block, mine, along_x(1))
            self.down = send(self.block, mine, along_x(3))
            self.across = send(self.block, mine, partner)
            self.full[fs] = self.block[...]

        def forward(self):
            prev = self.full.at[self.xs[3] * 2 + core]
            nxt = self.full.at[self.xs[1] * 2 + core]
            self.up.wait_recv()
            self.up2 = send(self.full.at[self.xs[3] * 2 + core, 0:half_rows], self.full.at[self.xs[3] * 2 + core, 0:half_rows], along_x(1))
            self.down.wait_recv()
            self.down2 = send(self.full.at[self.xs[1] * 2 + core, half_rows:], self.full.at[self.xs[1] * 2 + core, half_rows:], along_x(3))
            self.go(prev, partner)
            self.go(nxt, partner)

        def spread(self):
            self.up2.wait_recv()
            self.go(self.full.at[self.xs[2] * 2 + core, 0:half_rows], partner)
            self.down2.wait_recv()
            self.go(self.full.at[self.xs[2] * 2 + core, half_rows:], partner)

        def finish(self):
            self.across.wait_recv()
            for copy in self.copies:
                copy.wait_recv()
            for copy in self.copies + [self.up, self.down, self.across, self.up2, self.down2]:
                copy.wait_send()

    class Ring:
        def __init__(self, along, pos, part, bufs, sems=None):
            self.along, self.pos, self.part, self.bufs = along, pos, part, bufs

        def start(self):
            near, _ = self.bufs
            far = (self.pos + 2) % 4
            self.c = [send(self.part(far, 0), near.at[0], self.along(1)), send(self.part(far, 1), near.at[1], self.along(3))]

        def relay(self):
            near, full = self.bufs
            nxt, prev = (self.pos + 1) % 4, (self.pos + 3) % 4
            self.c[0].wait_recv()
            self.part(nxt, 0)[...] += near[0]
            self.c[1].wait_recv()
            self.part(prev, 1)[...] += near[1]
            self.c += [send(self.part(nxt, None), full.at[0], self.along(1)), send(self.part(prev, None), full.at[1], self.along(3))]

        def finish(self):
            _, full = self.bufs
            self.c[2].wait_recv()
            self.c[3].wait_recv()
            self.part(self.pos, None)[...] += full[0] + full[1]
            for copy in self.c:
                copy.wait_send()

    def piece(start, size, i, j):
        if j is None:
            return pl.ds(pl.multiple_of(start + size * i, 8), size)
        return pl.ds(pl.multiple_of(start + size * i + size // 2 * j, 8), size // 2)

    class Reduce:
        def __init__(self, grad, pair_in, out):
            self.grad, self.pair_in, self.out = grad, pair_in, out
            own = lambda i, rows: grad.at[i, core, rows]
            self.first = [Ring(along_x, my_x, lambda i, j: own(i, slice(0, half_rows) if j is None else slice(half_rows // 2 * j, half_rows // 2 * (j + 1))), (a1, a2)),
                          Ring(along_y, my_y, lambda i, j: grad.at[:, core, piece(half_rows, y_rows, i, j)], (b1, b2))]
            self.second = [Ring(along_y, my_y, lambda i, j: own(my_x, piece(0, y_rows, i, j)), (c1, c2)),
                           Ring(along_x, my_x, lambda i, j: own(i, piece(half_rows + y_rows * my_y, y_rows, 0, j)), (e1, e2))]

        def z_part(self, ref, h, z):
            return ref.at[pl.ds(pl.multiple_of(half_rows * h + y_rows * my_y + z_rows * z, 8), z_rows)]

        def y_part(self, h, pos):
            return self.out.at[pl.ds(pl.multiple_of(half_rows * h + y_rows * pos, 8), y_rows)]

        def r0(self):
            self.pair = [send(self.grad.at[i, other], self.pair_in(i), partner) for i in range(N_X)]

        def r1(self):
            for i in range(N_X):
                self.pair[i].wait_recv()

                def add(j, _):
                    s = pl.ds(pl.multiple_of(j * 128, 128), 128)
                    self.grad[i, core, s] += self.pair_in(i)[s]
                    return 0

                lax.fori_loop(0, d_model // 128, add, 0)
            for copy in self.pair:
                copy.wait_send()
            for ring in self.first:
                ring.start()

        def r2(self):
            for ring in self.first:
                ring.relay()

        def r3(self):
            for ring in self.first:
                ring.finish()
            for ring in self.second:
                ring.start()

        def r4(self):
            for ring in self.second:
                ring.relay()

        def r5(self):
            for ring in self.second:
                ring.finish()
            block = self.grad.at[my_x, core]
            self.z = [(i, h, send(self.z_part(block, h, (my_z + i) % N_Z), z_in.at[i - 1, h], along_z(i))) for i in range(1, N_Z) for h in range(2)]

        def r6(self):
            for _, _, copy in self.z:
                copy.wait_recv()
            block = self.grad.at[my_x, core]
            for h in range(2):
                total = self.z_part(block, h, my_z)[...]
                for i in range(1, N_Z):
                    total += z_in[i - 1, h]
                self.z_part(self.out, h, my_z)[...] = total * scale
            for _, _, copy in self.z:
                copy.wait_send()
            self.z = [(i, h, send(self.z_part(self.out, h, my_z), self.z_part(self.out, h, my_z), along_z(i))) for i in range(1, N_Z) for h in range(2)]

        def r7(self):
            for _, _, copy in self.z:
                copy.wait_recv()
            for _, _, copy in self.z:
                copy.wait_send()
            self.c = [send(self.y_part(h, my_y), self.y_part(h, my_y), along_y(i)) for i in (1, 3) for h in range(2)]

        def r8(self):
            for copy in self.c:
                copy.wait_recv()
            self.c += [send(self.y_part(0, (my_y + 3) % N_Y), self.y_part(0, (my_y + 3) % N_Y), along_y(1)),
                       send(self.y_part(1, (my_y + 1) % N_Y), self.y_part(1, (my_y + 1) % N_Y), along_y(3))]

        def r9(self):
            for copy in self.c[4:]:
                copy.wait_recv()
            for copy in self.c:
                copy.wait_send()

    class ReduceVec:
        def __init__(self):
            self.rows = vec_out.shape[0] // N_Z

        def part(self, ref, z):
            return ref.at[pl.ds(pl.multiple_of(self.rows * z, 8), self.rows)]

        def swap(self, slots, pos, along):
            return [send(slots.at[pos], slots.at[pos], along(i)) for i in range(1, 4)]

        def total(self, slots, copies):
            for copy in copies:
                copy.wait_recv()
            for copy in copies:
                copy.wait_send()
            return slots[0] + slots[1] + slots[2] + slots[3]

        def r1(self):
            for i in range(d_model // 128):
                vec_pair[0, 32 * i:32 * i + 32] = gv[:, 128 * i:128 * i + 128]
            self.c = [send(vec_pair.at[0], vec_pair.at[1], partner)]

        def r2(self):
            self.c[0].wait_recv()
            vec_x[my_x] = vec_pair[0] + vec_pair[1]
            self.c[0].wait_send()
            self.c = self.swap(vec_x, my_x, along_x)

        def r3(self):
            vec_y[my_y] = self.total(vec_x, self.c)
            self.c = self.swap(vec_y, my_y, along_y)

        def r5(self):
            vec_pair[0] = self.total(vec_y, self.c)
            self.c = [send(self.part(vec_pair.at[0], (my_z + i) % N_Z), vec_z.at[i - 1], along_z(i)) for i in range(1, N_Z)]

        def r6(self):
            for copy in self.c:
                copy.wait_recv()
            total = self.part(vec_pair.at[0], my_z)[...]
            for i in range(1, N_Z):
                total += vec_z[i - 1]
            self.part(vec_out, my_z)[...] = total * scale
            for copy in self.c:
                copy.wait_send()
            self.c = [send(self.part(vec_out, my_z), self.part(vec_out, my_z), along_z(i)) for i in range(1, N_Z)]

        def r7(self):
            for copy in self.c:
                copy.wait_recv()
            for copy in self.c:
                copy.wait_send()

    attn_gather, ffn_gather = Gather(attn_w, aw), Gather(ffn_w, fw)
    vec_copies = [send(vec_w, vec_all.at[fs], (dp, (fs + i) % (2 * N_X))) for i in range(1, 2 * N_X)]
    attn_gather.start()
    vec_all[fs] = vec_w[...]
    attn_gather.forward()
    ffn_gather.start()
    attn_gather.spread()
    for copy in vec_copies:
        copy.wait_recv()
    for copy in vec_copies:
        copy.wait_send()
    pair_rows = 19
    for i in range(N_X * pair_rows):
        p, r = i // pair_rows, i % pair_rows
        if r < 9:
            row = vec_all[2 * p, r:r + 1, :]
        elif r == 9:
            row = vec_all[2 * p, 9:10, :] + vec_all[2 * p + 1, 0:1, :]
        else:
            row = vec_all[2 * p + 1, r - 9:r - 8, :]
        vec[i // 4:i // 4 + 1, i % 4 * 128:i % 4 * 128 + 128] = row
    attn_gather.finish()

    ffn_reduce = Reduce(gf, lambda i: ga.at[i // 2, i % 2], ffn_out)
    attn_reduce = Reduce(ga, lambda i: gp.at[i, 0:d_model], attn_out)
    vec_reduce = ReduceVec()

    def rows(r):
        return pl.ds(pl.multiple_of(r * ROWS, ROWS), ROWS)

    def bias(i):
        return vec[i:i + 1, :]

    def add_vec(i, val):
        gv[pl.ds(i, 1), :] += jnp.sum(val, axis=0, keepdims=True)

    def norm(res):
        cen = res - jnp.mean(res, axis=-1, keepdims=True)
        inv = lax.rsqrt(jnp.mean(cen * cen, axis=-1, keepdims=True) + LN_EPS)
        return cen * inv, inv

    def norm_grad(d_out, normed, inv, slot):
        add_vec(slot, d_out * normed)
        add_vec(slot + 1, d_out)
        d_norm = d_out * bias(slot)
        return inv * (d_norm - jnp.mean(d_norm, axis=-1, keepdims=True) - normed * jnp.mean(d_norm * normed, axis=-1, keepdims=True))

    gv[...] = jnp.zeros_like(gv)

    def proj_self(r, _):
        s = rows(r)
        xr = x[s, :]
        er = enc[s, :]
        q[s, :] = ((mm(xr, aw[0]) + bias(0)) * 0.125).astype(BF)
        k[s, :] = (mm(xr, aw[1]) + bias(1)).astype(BF)
        v[s, :] = (mm(xr, aw[2]) + bias(2)).astype(BF)
        kc[s, :] = (mm(er, aw[5]) + bias(5)).astype(BF)
        vc[s, :] = (mm(er, aw[6]) + bias(6)).astype(BF)
        return 0

    lax.fori_loop(0, n_chunks, proj_self, 0)

    low_half = lax.broadcasted_iota(jnp.int32, (n_tgt, 128), 1) < 64

    def half(val, j):
        return jnp.where(low_half if j == 0 else ~low_half, val, jnp.zeros_like(val))

    def key_mask(b, causal):
        key_pos = lax.broadcasted_iota(jnp.int32, (n_tgt, n_src), 1)
        if causal:
            return (key_pos <= lax.broadcasted_iota(jnp.int32, (n_tgt, n_src), 0)) & (key_pos < tgt_lens[b])
        return key_pos < src_lens[b]

    def prob(qm, k2, mask):
        sc = jnp.where(mask, mm_nt(qm, k2), MASK_FILL)
        e = jnp.exp(sc - jnp.max(sc, axis=-1, keepdims=True))
        return e * (1.0 / jnp.sum(e, axis=-1, keepdims=True))

    def attn(q, k, v, o, causal):
        def step(i, _):
            b = i // n_pairs
            hp = i % n_pairs
            s = pl.ds(pl.multiple_of(b * n_tgt, n_tgt), n_tgt)
            c = pl.ds(pl.multiple_of(hp * 128, 128), 128)
            q2, k2, v2 = q[s, c], k[s, c], v[s, c]
            mask = key_mask(b, causal)
            outs = [mm(prob(half(q2, j), k2, mask).astype(BF), v2) for j in range(2)]
            o[s, c] = jnp.where(low_half, outs[0], outs[1]).astype(BF)
            return 0
        lax.fori_loop(0, n_batch * n_pairs, step, 0)

    def attn_grad(q, k, v, do, causal, part):
        def step(i, _):
            b = i // n_pairs
            hp = i % n_pairs
            s = pl.ds(pl.multiple_of(b * n_tgt, n_tgt), n_tgt)
            c = pl.ds(pl.multiple_of(hp * 128, 128), 128)
            q2, k2, v2, do2 = q[s, c], k[s, c], v[s, c], do[s, c]
            mask = key_mask(b, causal)
            qt, dot = q2.T, do2.T
            dq, dkt, dvt = [], [], []
            for j in range(2):
                p = prob(half(q2, j), k2, mask)
                dp = mm_nt(half(do2, j), v2)
                dvt.append(mm(dot[64 * j:64 * j + 64], p.astype(BF)))
                ds = (p * (dp - jnp.sum(p * dp, axis=-1, keepdims=True))).astype(BF)
                dq.append(mm(ds, k2))
                dkt.append(mm(qt[64 * j:64 * j + 64], ds))
            q[s, c] = (jnp.where(low_half, dq[0], dq[1]) * 0.125).astype(BF)
            k[s, c] = jnp.concatenate(dkt, axis=0).astype(BF).T
            v[s, c] = jnp.concatenate(dvt, axis=0).astype(BF).T
            return 0
        half_steps = n_batch * n_pairs // 2
        lax.fori_loop(part * half_steps, (part + 1) * half_steps, step, 0)

    attn(q, k, v, o, True)
    ffn_gather.forward()

    def post_self(r, _):
        s = rows(r)
        n1[s, :], i1[s, :] = norm(x[s, :].astype(F32) + mm(o[s, :], aw[3]) + bias(3))
        h = (n1[s, :] * bias(9) + bias(10)).astype(BF)
        h1[s, :] = h
        qc[s, :] = ((mm(h, aw[4]) + bias(4)) * 0.125).astype(BF)
        return 0

    lax.fori_loop(0, n_chunks, post_self, 0)
    attn(qc, kc, vc, oc, False)
    ffn_gather.spread()
    ffn_gather.finish()

    def ffn(r, _):
        s = rows(r)
        n2[s, :], i2[s, :] = norm(h1[s, :].astype(F32) + mm(oc[s, :], aw[7]) + bias(7))
        h = (n2[s, :] * bias(11) + bias(12)).astype(BF)
        h2[s, :] = h
        acc[s, :] = h.astype(F32) + bias(8)

        def up(f, _):
            u = mm_nt(h2[s, :], fw[f]) + vec[pl.ds(15 + f, 1), :]
            cdf = 0.5 * (1.0 + lax.erf(u * 0.7071067811865476))
            g_out = (u * cdf).astype(BF)
            g[f, s, :] = g_out
            gp[f, s, :] = cdf + u * (0.3989422804014327 * jnp.exp(-0.5 * u * u))
            acc[s, :] += mm(g_out, fw[n_ffn + f])
            return 0

        lax.fori_loop(0, n_ffn, up, 0)
        normed, inv = norm(acc[s, :])
        y[s, :] = (normed * bias(13) + bias(14)).astype(BF)
        d3 = norm_grad(dy[s, :].astype(F32), normed, inv, 13)
        add_vec(8, d3)
        dres[s, :] = d3
        dresb[s, :] = d3.astype(BF)
        return 0

    lax.fori_loop(0, n_chunks, ffn, 0)

    def ffn_grad(f, _):
        gf[(n_ffn + f) // 2, (n_ffn + f) % 2] = mm_tn(g[f], dresb[...])

        def up_grad(r, _):
            s = rows(r)
            d_up = mm_nt(dresb[s, :], fw[n_ffn + f]) * gp[f, s, :]
            add_vec(15 + f, d_up)
            d_up = d_up.astype(BF)
            g[f, s, :] = d_up
            dres[s, :] += mm(d_up, fw[f])
            return 0

        lax.fori_loop(0, n_chunks, up_grad, 0)
        gf[f // 2, f % 2] = mm_tn(g[f], h2[...])
        return 0

    lax.fori_loop(0, n_ffn, ffn_grad, 0)
    ffn_reduce.r0()

    def norm2_grad(r, _):
        s = rows(r)
        d2 = norm_grad(dres[s, :], n2[s, :], i2[s, :], 11)
        add_vec(7, d2)
        dres[s, :] = d2
        d2 = d2.astype(BF)
        dresb[s, :] = d2
        h2[s, :] = mm_nt(d2, aw[7]).astype(BF)
        return 0

    lax.fori_loop(0, n_chunks, norm2_grad, 0)
    ga[3, 1] = mm_tn(oc[...], dresb[...])
    attn_grad(qc, kc, vc, h2, False, 0)
    ffn_reduce.r1()
    attn_grad(qc, kc, vc, h2, False, 1)
    ffn_reduce.r2()
    ga[2, 0] = mm_tn(h1[...], qc[...])
    ga[2, 1] = mm_tn(enc[...], kc[...])
    ga[3, 0] = mm_tn(enc[...], vc[...])

    def norm1_grad(r, _):
        s = rows(r)
        add_vec(4, qc[s, :].astype(F32))
        add_vec(5, kc[s, :].astype(F32))
        add_vec(6, vc[s, :].astype(F32))
        denc[s, :] = (mm_nt(kc[s, :], aw[5]) + mm_nt(vc[s, :], aw[6])).astype(BF)
        d1 = norm_grad(dres[s, :] + mm_nt(qc[s, :], aw[4]), n1[s, :], i1[s, :], 9)
        add_vec(3, d1)
        dres[s, :] = d1
        d1 = d1.astype(BF)
        dresb[s, :] = d1
        h2[s, :] = mm_nt(d1, aw[3]).astype(BF)
        return 0

    lax.fori_loop(0, n_chunks, norm1_grad, 0)
    ga[1, 1] = mm_tn(o[...], dresb[...])
    attn_grad(q, k, v, h2, True, 0)
    ffn_reduce.r3()
    attn_grad(q, k, v, h2, True, 1)
    ffn_reduce.r4()
    ga[0, 0] = mm_tn(x[...], q[...])
    ga[0, 1] = mm_tn(x[...], k[...])
    ga[1, 0] = mm_tn(x[...], v[...])

    attn_reduce.r0()

    def last(r, _):
        s = rows(r)
        add_vec(0, q[s, :].astype(F32))
        add_vec(1, k[s, :].astype(F32))
        add_vec(2, v[s, :].astype(F32))
        dx[s, :] = (dres[s, :] + mm_nt(q[s, :], aw[0]) + mm_nt(k[s, :], aw[1]) + mm_nt(v[s, :], aw[2])).astype(BF)
        return 0

    lax.fori_loop(0, n_chunks, last, 0)
    ffn_reduce.r5()
    attn_reduce.r1()
    vec_reduce.r1()
    ffn_reduce.r6()
    vec_reduce.r2()
    attn_reduce.r2()
    vec_reduce.r3()
    attn_reduce.r3()
    attn_reduce.r4()
    vec_reduce.r5()
    ffn_reduce.r7()
    attn_reduce.r5()
    vec_reduce.r6()
    attn_reduce.r6()
    ffn_reduce.r8()
    vec_reduce.r7()
    attn_reduce.r7()
    ffn_reduce.r9()
    attn_reduce.r8()
    attn_reduce.r9()
    assert sem_count[0] <= send_sems.shape[0]


def solution(mesh):
    n_fsdp = mesh.shape['fsdp']
    n_dp = mesh.shape['dp']
    batch_axes = ('dp', 'fsdp')
    act_spec = P(batch_axes, None, None)
    len_spec = P(batch_axes)
    row_spec = P('fsdp', None)
    vec_spec = P('fsdp')

    def device_step(dec_in, enc_out, src_lens, tgt_lens, y_cot, attn_w, ffn_w, vec_params):
        n_batch, n_tgt, d = dec_in.shape
        n_src = enc_out.shape[1]
        n_tok = n_batch * n_tgt
        n_vec = vec_params.shape[0]
        ffn_dim = n_fsdp * ffn_w.shape[0] // 2
        n_ffn = ffn_dim // d
        scale = 1.0 / (n_tok * n_fsdp * n_dp)
        fs = lax.axis_index('fsdp')
        vec_f = vec_params.astype(F32)
        vec_w = jnp.where(fs % 2 == 0, jnp.pad(vec_f, (0, 2048 - n_vec)), jnp.pad(vec_f, (64, 2048 - 64 - n_vec))).reshape(16, 128)
        vm = pl.BlockSpec(memory_space=pltpu.VMEM)
        sm = pl.BlockSpec(memory_space=pltpu.SMEM)
        act = jax.ShapeDtypeStruct((n_tok, d), BF)
        block = jax.ShapeDtypeStruct((d, d), F32)
        buf = lambda *shape: pltpu.VMEM(shape, F32)
        tok = lambda dt: pltpu.VMEM((n_tok, d), dt)
        col = pltpu.VMEM((n_tok, 1), F32)
        weights = pltpu.VMEM((n_fsdp, d, d), BF)
        y, dx, denc, ga, gf, gv = pl.pallas_call(
            functools.partial(layer_kernel, n_batch, n_tgt, n_src, d, ffn_dim, scale),
            out_shape=(act, act, act, block, block, jax.ShapeDtypeStruct((128, 128), F32)),
            in_specs=[sm, sm] + [vm] * 6,
            out_specs=(vm,) * 6,
            scratch_shapes=[weights, weights, buf(N_X, 2, d, d), buf(N_X, 2, d, d), buf(32, d), buf(24, d), buf(n_fsdp, 16, 128)]
            + [tok(BF)] * 4 + [tok(BF), tok(F32), col] + [tok(BF)] * 4 + [tok(F32), col, tok(BF)]
            + [buf(n_ffn, n_tok, d), pltpu.VMEM((n_ffn, n_tok, d), BF), tok(F32), tok(BF)]
            + [buf(2, 128, d), buf(2, 256, d), buf(2, 4, 32, d), buf(2, 4, 64, d), buf(2, 32, d), buf(2, 64, d), buf(2, 32, d), buf(2, 64, d)]
            + [buf(7, 2, 8, d), buf(2, 128, 128), buf(4, 128, 128), buf(4, 128, 128), buf(7, 16, 128)]
            + [pltpu.SemaphoreType.DMA((160,)), pltpu.SemaphoreType.DMA((160,))],
            compiler_params=pltpu.CompilerParams(vmem_limit_bytes=67043328, collective_id=0, has_side_effects=True),
            cost_estimate=pl.CostEstimate(flops=24 * 10**9, bytes_accessed=30 * 2**20, transcendentals=0),
            name='layer',
        )(src_lens, tgt_lens, dec_in.reshape(n_tok, d), enc_out.reshape(n_tok, d), y_cot.reshape(n_tok, d), attn_w, ffn_w, vec_w)
        gv = gv.reshape(d // 128, 32, 128).transpose(1, 0, 2).reshape(-1)
        gv = lax.dynamic_slice_in_dim(gv, fs * n_vec, n_vec)
        return y.reshape(dec_in.shape), dx.reshape(dec_in.shape), denc.reshape(enc_out.shape), ga, gf, gv

    return jax.shard_map(device_step, mesh=mesh, in_specs=(act_spec, act_spec, len_spec, len_spec, act_spec, row_spec, row_spec, vec_spec), out_specs=(act_spec, act_spec, act_spec, row_spec, row_spec, vec_spec), check_vma=False)
```

```python
import functools
import jax
import jax.numpy as jnp
from jax import lax
from jax.experimental import pallas as pl
from jax.experimental.pallas import tpu as pltpu
from jax.sharding import PartitionSpec as P

LN_EPS = 1e-5
MASK_FILL = -1e30
BF = jnp.bfloat16
F32 = jnp.float32
ROWS = 256


def mm(a, b):
    return lax.dot_general(a, b, (((1,), (0,)), ((), ())), preferred_element_type=F32)


def mm_nt(a, b):
    return lax.dot_general(a, b, (((1,), (1,)), ((), ())), preferred_element_type=F32)


def mm_tn(a, b):
    return lax.dot_general(a, b, (((0,), (0,)), ((), ())), preferred_element_type=F32)


N_X = 4
N_Y = 4
N_Z = 8
MESH = pl.DeviceIdType.MESH
FFN_PLAN = ((True, 256), (False, 256))
ATTN_PLAN = ((False, 128), (True, 128), (False, 128), (True, 128))


def layer_kernel(n_batch, n_tgt, n_src, d_model, ffn_dim, scale, src_lens, tgt_lens, x_any, enc_any, dy_any, attn_w, ffn_w, vec_w,
                 y_any, dx_any, denc_any, attn_out, ffn_out, vec_out,
                 x, enc, dy, y, dx, denc, local_sems,
                 aw, fw, ga, gf, gv, vec, vec_all, q, k, v, o, h1, n1, i1, qc, kc, vc, oc, n2, i2, h2, gp, g, dres, dresb,
                 a1, a2, c1, c2, z_x, b1, b2, e1, e2, z_y, vec_pair, vec_x, vec_y, vec_z, send_sems, recv_sems):
    acc = dres
    n_ffn = ffn_dim // d_model
    n_tok = n_batch * n_tgt
    n_chunks = n_tok // ROWS
    n_pairs = d_model // 128
    half_rows = d_model // 2
    y_rows = d_model // N_Y
    x_bufs, y_bufs = (a1, a2, c1, c2, z_x), (b1, b2, e1, e2, z_y)
    z_rows = y_rows // N_Z

    dp = lax.axis_index('dp')
    fs = lax.axis_index('fsdp')
    my_z, my_y = dp // N_Y, dp % N_Y
    my_x, core = fs // 2, fs % 2
    other = 1 - core
    sem_count = [0]

    def along_x(step):
        return (dp, (my_x + step) % N_X * 2 + core)

    def along_y(step):
        return (my_z * N_Y + (my_y + step) % N_Y, fs)

    def along_z(step):
        return ((my_z + step) % N_Z * N_Y + my_y, fs)

    partner = (dp, my_x * 2 + other)

    def new_sem():
        sem_count[0] += 1
        return sem_count[0] - 1

    def remote(src, dst, sem, device):
        return pltpu.make_async_remote_copy(src_ref=src, dst_ref=dst, send_sem=send_sems.at[sem], recv_sem=recv_sems.at[sem], device_id=device, device_id_type=MESH)

    def send(src, dst, device):
        copy = remote(src, dst, new_sem(), device)
        copy.start()
        return copy

    loads = [pltpu.make_async_copy(src, dst, local_sems.at[i]) for i, (src, dst) in enumerate(((x_any, x), (enc_any, enc), (dy_any, dy)))]
    stores = [pltpu.make_async_copy(src, dst, local_sems.at[3 + i]) for i, (src, dst) in enumerate(((y, y_any), (dx, dx_any), (denc, denc_any)))]
    for load in loads:
        load.start()
    barrier = pltpu.get_barrier_semaphore()
    peers = [(dp, (fs + i) % (2 * N_X)) for i in range(1, 2 * N_X)]
    peers += [along_y(i) for i in range(1, N_Y)] + [along_z(i) for i in range(1, N_Z)]
    for peer in peers:
        pl.semaphore_signal(barrier, inc=1, device_id=peer, device_id_type=MESH)
    pl.semaphore_wait(barrier, len(peers))

    class Gather:
        def __init__(self, block, full):
            self.block, self.full, self.copies = block, full, []
            self.xs = [(my_x + i) % N_X for i in range(N_X)]

        def go(self, src, device):
            self.copies.append(send(src, src, device))
            return self.copies[-1]

        def half(self, ref, j):
            return ref.at[half_rows * j:half_rows * (j + 1)]

        def slot(self, step, j):
            return self.half(self.full.at[self.xs[step] * 2 + core], j)

        def start(self):
            mine = self.full.at[fs]
            self.first = [send(self.half(self.block, j), self.half(mine, j), along_x(1 + 2 * j)) for j in range(2)]
            self.second = [send(self.half(self.block, 1 - j), self.half(mine, 1 - j), along_x(1 + 2 * j)) for j in range(2)]
            self.across = send(self.block, mine, partner)
            self.full[fs] = self.block[...]

        def forward(self):
            self.hop = []
            for j, came in ((0, 3), (1, 1)):
                self.first[j].wait_recv()
                self.hop.append(send(self.slot(came, j), self.slot(came, j), along_x(1 + 2 * j)))
                self.go(self.slot(came, j), partner)
            for j, came in ((0, 3), (1, 1)):
                self.second[j].wait_recv()
                self.go(self.slot(came, 1 - j), partner)

        def spread(self):
            for j in range(2):
                self.hop[j].wait_recv()
                self.go(self.slot(2, j), partner)

        def finish(self):
            self.across.wait_recv()
            for copy in self.copies:
                copy.wait_recv()
            for copy in self.copies + self.first + self.second + self.hop + [self.across]:
                copy.wait_send()

    class Ring:
        def __init__(self, along, pos, part, near, full):
            self.along, self.pos, self.part, self.near, self.full = along, pos, part, near, full
            self.far, self.nxt, self.prev = (pos + 2) % 4, (pos + 1) % 4, (pos + 3) % 4

        def start(self):
            self.c = [send(self.part(self.far, 0), self.near(0), self.along(1)), send(self.part(self.far, 1), self.near(1), self.along(3))]

        def direct(self):
            self.c += [send(self.part(self.nxt, 1), self.full(0, 1), self.along(1)), send(self.part(self.prev, 0), self.full(1, 0), self.along(3))]

        def relay(self):
            for way, target in ((0, self.nxt), (1, self.prev)):
                self.c[way].wait_recv()
                self.part(target, way)[...] += self.near(way)[...]
                self.c.append(send(self.part(target, way), self.full(way, way), self.along(1 + 2 * way)))

        def finish(self):
            for copy in self.c[2:]:
                copy.wait_recv()
            self.part(self.pos, None)[...] += self.full(0, None)[...] + self.full(1, None)[...]
            for copy in self.c:
                copy.wait_send()

    def split(start, size, j):
        if j is None:
            return pl.ds(pl.multiple_of(start, 8), size)
        return pl.ds(pl.multiple_of(start + size // 2 * j, 8), size // 2)

    class Reduce:
        def __init__(self, grad, pair_in, out, x_first, lane, width, spare):
            self.out = out
            self.cols = cols = slice(lane, lane + width)
            self.lands = lands = slice(spare, spare + width)
            self.block = grad.at[core, my_x]
            bufs = x_bufs if x_first else y_bufs
            self.z_in = bufs[4]
            near_in = lambda k: (lambda way: bufs[k].at[way, ..., lands])
            full_in = lambda k: (lambda way, j: bufs[k].at[(way,) + (slice(None),) * (len(bufs[k].shape) - 3) + (split(0, bufs[k].shape[-2], j), lands)])
            if x_first:
                part_of = lambda c: (lambda i, j: grad.at[c, i, split(0, d_model, j), cols])
                first = (along_x, my_x)
                self.second = Ring(along_y, my_y, lambda i, j: grad.at[core, my_x, split(y_rows * i, y_rows, j), cols], near_in(2), full_in(3))
                self.pair_part = lambda i: pair_in(i, slice(0, d_model), cols)
            else:
                part_of = lambda c: (lambda i, j: grad.at[c, :, split(y_rows * i, y_rows, j), cols])
                first = (along_y, my_y)
                self.second = Ring(along_x, my_x, lambda i, j: grad.at[core, i, split(y_rows * my_y, y_rows, j), cols], near_in(2), full_in(3))
                self.pair_part = lambda i: pair_in(slice(None), split(y_rows * i, y_rows, None), cols)
            self.first = Ring(*first, part_of(core), near_in(0), full_in(1))
            self.pair_src = part_of(other)
            self.pair = {}

        def rows_at(self, ref, start, size):
            return ref.at[pl.ds(pl.multiple_of(start, 8), size), self.cols]

        def z_part(self, ref, z):
            return self.rows_at(ref, y_rows * my_y + z_rows * z, z_rows)

        def y_part(self, pos, half=None):
            return self.out.at[split(y_rows * pos, y_rows, half), self.cols]

        def swap(self, name):
            i = getattr(self.first, name)
            self.pair[name] = send(self.pair_src(i, None), self.pair_part(i), partner)

        def merge(self, name):
            i = getattr(self.first, name)
            self.pair[name].wait_recv()
            self.first.part(i, None)[...] += self.pair_part(i)[...]

        def r1(self):
            self.merge('far')
            self.first.start()

        def r1b(self):
            self.merge('nxt')
            self.merge('prev')
            self.first.direct()

        def r2(self):
            self.first.relay()
            self.merge('pos')

        def r3(self):
            for copy in self.pair.values():
                copy.wait_send()
            self.first.finish()
            self.second.start()
            self.second.direct()

        def r4(self):
            self.second.relay()

        def r5(self):
            self.second.finish()
            self.z = [send(self.z_part(self.block, (my_z + i) % N_Z), self.z_in.at[i - 1, :, self.lands], along_z(i)) for i in range(1, N_Z)]

        def r6(self):
            for copy in self.z:
                copy.wait_recv()
            total = self.z_part(self.block, my_z)[...]
            for i in range(1, N_Z):
                total += self.z_in[i - 1, :, self.lands]
            self.z_part(self.out, my_z)[...] = total * scale
            for copy in self.z:
                copy.wait_send()
            self.z = [send(self.z_part(self.out, my_z), self.z_part(self.out, my_z), along_z(i)) for i in range(1, N_Z)]

        def r7(self):
            for copy in self.z:
                copy.wait_recv()
            for copy in self.z:
                copy.wait_send()
            self.c = [send(self.y_part(my_y), self.y_part(my_y), along_y(i)) for i in (1, 3)]

        def r8(self):
            for way, pos in ((0, (my_y + 3) % N_Y), (1, (my_y + 1) % N_Y)):
                self.c[way].wait_recv()
                self.c.append(send(self.y_part(pos, way), self.y_part(pos, way), along_y(1 + 2 * way)))

        def r9(self):
            for copy in self.c[2:]:
                copy.wait_recv()
            for copy in self.c:
                copy.wait_send()

    class Group:
        def __init__(self, parts):
            self.parts = parts

        def r0(self):
            for name in ('far', 'nxt', 'prev', 'pos'):
                for part in self.parts:
                    part.swap(name)

        def __getattr__(self, name):
            def call():
                for part in self.parts:
                    getattr(part, name)()
            return call

    def reduce_all(grad, pair_in, out, plan):
        used = {True: 0, False: 0}
        parts = []
        lane = 0
        for x_first, width in plan:
            parts.append(Reduce(grad, pair_in, out, x_first, lane, width, used[x_first]))
            used[x_first] += width
            lane += width
        return Group(parts)

    class ReduceVec:
        def __init__(self):
            self.rows = vec_out.shape[0] // N_Z

        def part(self, ref, z):
            return ref.at[pl.ds(pl.multiple_of(self.rows * z, 8), self.rows)]

        def swap(self, slots, pos, along):
            return [send(slots.at[pos], slots.at[pos], along(i)) for i in range(1, 4)]

        def total(self, slots, copies):
            for copy in copies:
                copy.wait_recv()
            for copy in copies:
                copy.wait_send()
            return slots[0] + slots[1] + slots[2] + slots[3]

        def r1(self):
            for i in range(d_model // 128):
                vec_pair[0, 32 * i:32 * i + 32] = gv[:, 128 * i:128 * i + 128]
            self.c = [send(vec_pair.at[0], vec_pair.at[1], partner)]

        def r2(self):
            self.c[0].wait_recv()
            vec_x[my_x] = vec_pair[0] + vec_pair[1]
            self.c[0].wait_send()
            self.c = self.swap(vec_x, my_x, along_x)

        def r3(self):
            vec_y[my_y] = self.total(vec_x, self.c)
            self.c = self.swap(vec_y, my_y, along_y)

        def r5(self):
            vec_pair[0] = self.total(vec_y, self.c)
            self.c = [send(self.part(vec_pair.at[0], (my_z + i) % N_Z), vec_z.at[i - 1], along_z(i)) for i in range(1, N_Z)]

        def r6(self):
            for copy in self.c:
                copy.wait_recv()
            total = self.part(vec_pair.at[0], my_z)[...]
            for i in range(1, N_Z):
                total += vec_z[i - 1]
            self.part(vec_out, my_z)[...] = total * scale
            for copy in self.c:
                copy.wait_send()
            self.c = [send(self.part(vec_out, my_z), self.part(vec_out, my_z), along_z(i)) for i in range(1, N_Z)]

        def r7(self):
            for copy in self.c:
                copy.wait_recv()
            for copy in self.c:
                copy.wait_send()

    attn_gather, ffn_gather = Gather(attn_w, aw), Gather(ffn_w, fw)
    vec_copies = [send(vec_w, vec_all.at[fs], (dp, (fs + i) % (2 * N_X))) for i in range(1, 2 * N_X)]
    attn_gather.start()
    vec_all[fs] = vec_w[...]
    attn_gather.forward()
    ffn_gather.start()
    attn_gather.spread()
    for copy in vec_copies:
        copy.wait_recv()
    for copy in vec_copies:
        copy.wait_send()
    pair_rows = 19
    for i in range(N_X * pair_rows):
        p, r = i // pair_rows, i % pair_rows
        if r < 9:
            row = vec_all[2 * p, r:r + 1, :]
        elif r == 9:
            row = vec_all[2 * p, 9:10, :] + vec_all[2 * p + 1, 0:1, :]
        else:
            row = vec_all[2 * p + 1, r - 9:r - 8, :]
        vec[i // 4:i // 4 + 1, i % 4 * 128:i % 4 * 128 + 128] = row
    attn_gather.finish()
    for load in loads:
        load.wait()

    ffn_reduce = reduce_all(gf, lambda i, r, c: ga.at[0, i, r, c], ffn_out, FFN_PLAN)
    attn_reduce = reduce_all(ga, lambda i, r, c: gp.at[i, r, c], attn_out, ATTN_PLAN)
    vec_reduce = ReduceVec()

    def rows(r):
        return pl.ds(pl.multiple_of(r * ROWS, ROWS), ROWS)

    def bias(i):
        return vec[i:i + 1, :]

    def add_vec(i, val):
        gv[pl.ds(i, 1), :] += jnp.sum(val, axis=0, keepdims=True)

    def norm(res):
        cen = res - jnp.mean(res, axis=-1, keepdims=True)
        inv = lax.rsqrt(jnp.mean(cen * cen, axis=-1, keepdims=True) + LN_EPS)
        return cen * inv, inv

    def norm_grad(d_out, normed, inv, slot):
        add_vec(slot, d_out * normed)
        add_vec(slot + 1, d_out)
        d_norm = d_out * bias(slot)
        return inv * (d_norm - jnp.mean(d_norm, axis=-1, keepdims=True) - normed * jnp.mean(d_norm * normed, axis=-1, keepdims=True))

    gv[...] = jnp.zeros_like(gv)

    def proj_self(r, _):
        s = rows(r)
        xr = x[s, :]
        er = enc[s, :]
        q[s, :] = ((mm(xr, aw[0]) + bias(0)) * 0.125).astype(BF)
        k[s, :] = (mm(xr, aw[1]) + bias(1)).astype(BF)
        v[s, :] = (mm(xr, aw[2]) + bias(2)).astype(BF)
        kc[s, :] = (mm(er, aw[5]) + bias(5)).astype(BF)
        vc[s, :] = (mm(er, aw[6]) + bias(6)).astype(BF)
        return 0

    lax.fori_loop(0, n_chunks, proj_self, 0)

    low_half = lax.broadcasted_iota(jnp.int32, (n_tgt, 128), 1) < 64

    def half(val, j):
        return jnp.where(low_half if j == 0 else ~low_half, val, jnp.zeros_like(val))

    def key_mask(b, causal):
        key_pos = lax.broadcasted_iota(jnp.int32, (n_tgt, n_src), 1)
        if causal:
            return (key_pos <= lax.broadcasted_iota(jnp.int32, (n_tgt, n_src), 0)) & (key_pos < tgt_lens[b])
        return key_pos < src_lens[b]

    def prob(qm, k2, mask):
        sc = jnp.where(mask, mm_nt(qm, k2), MASK_FILL)
        e = jnp.exp(sc - jnp.max(sc, axis=-1, keepdims=True))
        return e * (1.0 / jnp.sum(e, axis=-1, keepdims=True))

    def attn(q, k, v, o, causal):
        def step(i, _):
            b = i // n_pairs
            hp = i % n_pairs
            s = pl.ds(pl.multiple_of(b * n_tgt, n_tgt), n_tgt)
            c = pl.ds(pl.multiple_of(hp * 128, 128), 128)
            q2, k2, v2 = q[s, c], k[s, c], v[s, c]
            mask = key_mask(b, causal)
            outs = [mm(prob(half(q2, j), k2, mask).astype(BF), v2) for j in range(2)]
            o[s, c] = jnp.where(low_half, outs[0], outs[1]).astype(BF)
            return 0
        lax.fori_loop(0, n_batch * n_pairs, step, 0)

    def attn_grad(q, k, v, do, causal, begin, end):
        def step(i, _):
            b = i // n_pairs
            hp = i % n_pairs
            s = pl.ds(pl.multiple_of(b * n_tgt, n_tgt), n_tgt)
            c = pl.ds(pl.multiple_of(hp * 128, 128), 128)
            q2, k2, v2, do2 = q[s, c], k[s, c], v[s, c], do[s, c]
            mask = key_mask(b, causal)
            qt, dot = q2.T, do2.T
            dq, dkt, dvt = [], [], []
            for j in range(2):
                p = prob(half(q2, j), k2, mask)
                dp = mm_nt(half(do2, j), v2)
                dvt.append(mm(dot[64 * j:64 * j + 64], p.astype(BF)))
                ds = (p * (dp - jnp.sum(p * dp, axis=-1, keepdims=True))).astype(BF)
                dq.append(mm(ds, k2))
                dkt.append(mm(qt[64 * j:64 * j + 64], ds))
            q[s, c] = (jnp.where(low_half, dq[0], dq[1]) * 0.125).astype(BF)
            k[s, c] = jnp.concatenate(dkt, axis=0).astype(BF).T
            v[s, c] = jnp.concatenate(dvt, axis=0).astype(BF).T
            return 0
        steps = n_batch * n_pairs
        lax.fori_loop(begin * steps // 4, end * steps // 4, step, 0)

    attn(q, k, v, o, True)
    ffn_gather.forward()

    def post_self(r, _):
        s = rows(r)
        n1[s, :], i1[s, :] = norm(x[s, :].astype(F32) + mm(o[s, :], aw[3]) + bias(3))
        h = (n1[s, :] * bias(9) + bias(10)).astype(BF)
        h1[s, :] = h
        qc[s, :] = ((mm(h, aw[4]) + bias(4)) * 0.125).astype(BF)
        return 0

    lax.fori_loop(0, n_chunks, post_self, 0)
    attn(qc, kc, vc, oc, False)
    ffn_gather.spread()
    ffn_gather.finish()

    def ffn(r, _):
        s = rows(r)
        n2[s, :], i2[s, :] = norm(h1[s, :].astype(F32) + mm(oc[s, :], aw[7]) + bias(7))
        h = (n2[s, :] * bias(11) + bias(12)).astype(BF)
        h2[s, :] = h
        acc[s, :] = h.astype(F32) + bias(8)

        def up(f, _):
            u = mm_nt(h2[s, :], fw[f]) + vec[pl.ds(15 + f, 1), :]
            cdf = 0.5 * (1.0 + lax.erf(u * 0.7071067811865476))
            g_out = (u * cdf).astype(BF)
            g[f, s, :] = g_out
            gp[f, s, :] = cdf + u * (0.3989422804014327 * jnp.exp(-0.5 * u * u))
            acc[s, :] += mm(g_out, fw[n_ffn + f])
            return 0

        lax.fori_loop(0, n_ffn, up, 0)
        normed, inv = norm(acc[s, :])
        y[s, :] = (normed * bias(13) + bias(14)).astype(BF)
        d3 = norm_grad(dy[s, :].astype(F32), normed, inv, 13)
        add_vec(8, d3)
        dres[s, :] = d3
        dresb[s, :] = d3.astype(BF)
        return 0

    lax.fori_loop(0, n_chunks, ffn, 0)
    stores[0].start()

    def ffn_grad(f, _):
        gf[(n_ffn + f) % 2, (n_ffn + f) // 2] = mm_tn(g[f], dresb[...])

        def up_grad(r, _):
            s = rows(r)
            d_up = mm_nt(dresb[s, :], fw[n_ffn + f]) * gp[f, s, :]
            add_vec(15 + f, d_up)
            d_up = d_up.astype(BF)
            g[f, s, :] = d_up
            dres[s, :] += mm(d_up, fw[f])
            return 0

        lax.fori_loop(0, n_chunks, up_grad, 0)
        gf[f % 2, f // 2] = mm_tn(g[f], h2[...])
        return 0

    lax.fori_loop(0, n_ffn, ffn_grad, 0)
    ffn_reduce.r0()

    def norm2_grad(r, _):
        s = rows(r)
        d2 = norm_grad(dres[s, :], n2[s, :], i2[s, :], 11)
        add_vec(7, d2)
        dres[s, :] = d2
        d2 = d2.astype(BF)
        dresb[s, :] = d2
        h2[s, :] = mm_nt(d2, aw[7]).astype(BF)
        return 0

    lax.fori_loop(0, n_chunks, norm2_grad, 0)
    ga[1, 3] = mm_tn(oc[...], dresb[...])
    ffn_reduce.r1()
    ffn_reduce.r1b()
    attn_grad(qc, kc, vc, h2, False, 0, 2)
    ffn_reduce.r2()
    attn_grad(qc, kc, vc, h2, False, 2, 4)
    ga[0, 2] = mm_tn(h1[...], qc[...])
    ga[1, 2] = mm_tn(enc[...], kc[...])
    ga[0, 3] = mm_tn(enc[...], vc[...])

    def norm1_grad(r, _):
        s = rows(r)
        d1 = norm_grad(dres[s, :] + mm_nt(qc[s, :], aw[4]), n1[s, :], i1[s, :], 9)
        add_vec(3, d1)
        dres[s, :] = d1
        d1 = d1.astype(BF)
        dresb[s, :] = d1
        h2[s, :] = mm_nt(d1, aw[3]).astype(BF)
        return 0

    lax.fori_loop(0, n_chunks, norm1_grad, 0)
    ga[1, 1] = mm_tn(o[...], dresb[...])
    attn_grad(q, k, v, h2, True, 0, 2)
    ffn_reduce.r3()
    attn_grad(q, k, v, h2, True, 2, 3)
    ffn_reduce.r4()
    attn_grad(q, k, v, h2, True, 3, 4)
    ffn_reduce.r5()
    ga[0, 0] = mm_tn(x[...], q[...])
    ga[1, 0] = mm_tn(x[...], k[...])
    ga[0, 1] = mm_tn(x[...], v[...])

    attn_reduce.r0()
    ffn_reduce.r6()
    attn_reduce.r1()
    attn_reduce.r1b()

    def last(r, _):
        s = rows(r)
        add_vec(4, qc[s, :].astype(F32))
        add_vec(5, kc[s, :].astype(F32))
        add_vec(6, vc[s, :].astype(F32))
        denc[s, :] = (mm_nt(kc[s, :], aw[5]) + mm_nt(vc[s, :], aw[6])).astype(BF)
        add_vec(0, q[s, :].astype(F32))
        add_vec(1, k[s, :].astype(F32))
        add_vec(2, v[s, :].astype(F32))
        dx[s, :] = (dres[s, :] + mm_nt(q[s, :], aw[0]) + mm_nt(k[s, :], aw[1]) + mm_nt(v[s, :], aw[2])).astype(BF)
        return 0

    lax.fori_loop(0, n_chunks, last, 0)
    stores[1].start()
    stores[2].start()
    vec_reduce.r1()
    ffn_reduce.r7()
    attn_reduce.r2()
    vec_reduce.r2()
    attn_reduce.r3()
    vec_reduce.r3()
    ffn_reduce.r8()
    attn_reduce.r4()
    vec_reduce.r5()
    attn_reduce.r5()
    attn_reduce.r6()
    vec_reduce.r6()
    attn_reduce.r7()
    vec_reduce.r7()
    ffn_reduce.r9()
    attn_reduce.r8()
    attn_reduce.r9()
    for store in stores:
        store.wait()
    assert sem_count[0] <= send_sems.shape[0]


def copy_out(*refs):
    for src, dst in zip(refs[:5], refs[5:]):
        dst[...] = src[...]


def solution(mesh):
    n_fsdp = mesh.shape['fsdp']
    n_dp = mesh.shape['dp']
    batch_axes = ('dp', 'fsdp')
    act_spec = P(batch_axes, None, None)
    len_spec = P(batch_axes)
    row_spec = P('fsdp', None)
    vec_spec = P('fsdp')

    def device_step(dec_in, enc_out, src_lens, tgt_lens, y_cot, attn_w, ffn_w, vec_params):
        n_batch, n_tgt, d = dec_in.shape
        n_src = enc_out.shape[1]
        n_tok = n_batch * n_tgt
        n_vec = vec_params.shape[0]
        ffn_dim = n_fsdp * ffn_w.shape[0] // 2
        n_ffn = ffn_dim // d
        scale = 1.0 / (n_tok * n_fsdp * n_dp)
        fs = lax.axis_index('fsdp')
        vec_f = vec_params.astype(F32)
        vec_w = jnp.where(fs % 2 == 0, jnp.pad(vec_f, (0, 2048 - n_vec)), jnp.pad(vec_f, (64, 2048 - 64 - n_vec))).reshape(16, 128)
        vm = pl.BlockSpec(memory_space=pltpu.VMEM)
        hbm = pl.BlockSpec(memory_space=pl.ANY)
        sm = pl.BlockSpec(memory_space=pltpu.SMEM)
        act = jax.ShapeDtypeStruct((n_tok, d), BF)
        block = jax.ShapeDtypeStruct((d, d), F32)
        buf = lambda *shape: pltpu.VMEM(shape, F32)
        tok = lambda dt: pltpu.VMEM((n_tok, d), dt)
        col = pltpu.VMEM((n_tok, 1), F32)
        weights = pltpu.VMEM((n_fsdp, d, d), BF)
        y, dx, denc, ga, gf, gv = pl.pallas_call(
            functools.partial(layer_kernel, n_batch, n_tgt, n_src, d, ffn_dim, scale),
            out_shape=(act, act, act, block, block, jax.ShapeDtypeStruct((128, 128), F32)),
            in_specs=[sm, sm] + [hbm] * 3 + [vm] * 3,
            out_specs=(hbm,) * 3 + (vm,) * 3,
            scratch_shapes=[tok(BF)] * 6 + [pltpu.SemaphoreType.DMA((6,)), weights, weights, buf(2, N_X, d, d), buf(2, N_X, d, d), buf(32, d), buf(24, d), buf(n_fsdp, 16, 128)]
            + [tok(BF)] * 4 + [tok(BF), tok(F32), col] + [tok(BF)] * 4 + [tok(F32), col, tok(BF)]
            + [buf(n_ffn, n_tok, d), pltpu.VMEM((n_ffn, n_tok, d), BF), tok(F32), tok(BF)]
            + [buf(2, d // 2, 256), buf(2, d, 256), buf(2, 64, 256), buf(2, 128, 256), buf(7, 16, 256)]
            + [buf(2, N_X, 64, 256), buf(2, N_X, 128, 256), buf(2, 64, 256), buf(2, 128, 256), buf(7, 16, 256)]
            + [buf(2, 128, 128), buf(4, 128, 128), buf(4, 128, 128), buf(7, 16, 128)]
            + [pltpu.SemaphoreType.DMA((260,)), pltpu.SemaphoreType.DMA((260,))],
            compiler_params=pltpu.CompilerParams(vmem_limit_bytes=67043328, collective_id=0, has_side_effects=True),
            cost_estimate=pl.CostEstimate(flops=24 * 10**9, bytes_accessed=30 * 2**20, transcendentals=0),
            name='layer',
        )(src_lens, tgt_lens, dec_in.reshape(n_tok, d), enc_out.reshape(n_tok, d), y_cot.reshape(n_tok, d), attn_w, ffn_w, vec_w)
        n_steps = 4
        tiles = [pl.BlockSpec((arr.shape[0] // n_steps, d), lambda i: (i, 0)) for arr in (y, dx, denc, ga, gf)]
        y, dx, denc, ga, gf = pl.pallas_call(
            copy_out,
            grid=(n_steps,),
            out_shape=tuple(jax.ShapeDtypeStruct(arr.shape, arr.dtype) for arr in (y, dx, denc, ga, gf)),
            in_specs=tiles,
            out_specs=tuple(tiles),
            compiler_params=pltpu.CompilerParams(vmem_limit_bytes=67043328),
            name='out',
        )(y, dx, denc, ga, gf)
        gv = gv.reshape(d // 128, 32, 128).transpose(1, 0, 2).reshape(-1)
        gv = lax.dynamic_slice_in_dim(gv, fs * n_vec, n_vec)
        return y.reshape(dec_in.shape), dx.reshape(dec_in.shape), denc.reshape(enc_out.shape), ga, gf, gv

    return jax.shard_map(device_step, mesh=mesh, in_specs=(act_spec, act_spec, len_spec, len_spec, act_spec, row_spec, row_spec, vec_spec), out_specs=(act_spec, act_spec, act_spec, row_spec, row_spec, vec_spec), check_vma=False)
```

```python
import functools
import jax
import jax.numpy as jnp
from jax import lax
from jax.experimental import pallas as pl
from jax.experimental.pallas import tpu as pltpu
from jax.sharding import PartitionSpec as P

LN_EPS = 1e-5
MASK_FILL = -1e30
BF = jnp.bfloat16
F32 = jnp.float32
ROWS = 768


def mm(a, b):
    return lax.dot_general(a, b, (((1,), (0,)), ((), ())), preferred_element_type=F32)


def mm_nt(a, b):
    return lax.dot_general(a, b, (((1,), (1,)), ((), ())), preferred_element_type=F32)


def mm_tn(a, b):
    return lax.dot_general(a, b, (((0,), (0,)), ((), ())), preferred_element_type=F32)


N_X = 4
N_Y = 4
N_Z = 8
MESH = pl.DeviceIdType.MESH
ALL = slice(None)
FFN_PLAN = ((True, 256), (False, 256))
ATTN_PLAN = ((False, 128), (True, 128), (False, 128), (True, 128))


def layer_kernel(n_batch, n_tgt, n_src, d_model, ffn_dim, scale, src_lens, tgt_lens, x_any, enc_any, dy_any, attn_w, ffn_w, vec_w,
                 y_any, dx_any, denc_any, attn_out, ffn_out, vec_out,
                 x, enc, dy, y, denc, local_sems,
                 aw, fw, ga, gf, gv, vec, vec_all, q, k, v, o, h1, n1, i1, qc, kc, vc, oc, n2, i2, h2, gp, g, dres, dresb,
                 a1, a2, c1, c2, z_x, b1, b2, e1, e2, z_y, vec_pair, vec_x, vec_y, vec_z, send_sems, recv_sems):
    acc, dx = dres, dy
    n_ffn = ffn_dim // d_model
    n_tok = n_batch * n_tgt
    n_chunks = n_tok // ROWS
    n_pairs = d_model // 128
    half_rows = d_model // 2
    y_rows = d_model // N_Y
    x_bufs, y_bufs = (a1, a2, c1, c2, z_x), (b1, b2, e1, e2, z_y)
    z_rows = y_rows // N_Z

    dp = lax.axis_index('dp')
    fs = lax.axis_index('fsdp')
    my_z, my_y = dp // N_Y, dp % N_Y
    my_x, core = fs // 2, fs % 2
    other = 1 - core
    sem_count = [0]

    def along_x(step):
        return (dp, (my_x + step) % N_X * 2 + core)

    def along_y(step):
        return (my_z * N_Y + (my_y + step) % N_Y, fs)

    def along_z(step):
        return ((my_z + step) % N_Z * N_Y + my_y, fs)

    partner = (dp, my_x * 2 + other)

    def new_sem():
        sem_count[0] += 1
        return sem_count[0] - 1

    def remote(src, dst, sem, device):
        return pltpu.make_async_remote_copy(src_ref=src, dst_ref=dst, send_sem=send_sems.at[sem], recv_sem=recv_sems.at[sem], device_id=device, device_id_type=MESH)

    def send(src, dst, device):
        copy = remote(src, dst, new_sem(), device)
        copy.start()
        return copy

    loads = [pltpu.make_async_copy(src, dst, local_sems.at[i]) for i, (src, dst) in enumerate(((x_any, x), (enc_any, enc), (dy_any, dy)))]
    stores = [pltpu.make_async_copy(src, dst, local_sems.at[3 + i]) for i, (src, dst) in enumerate(((y, y_any), (dx, dx_any), (denc, denc_any)))]
    for load in loads:
        load.start()
    barrier = pltpu.get_barrier_semaphore()
    peers = [(dp, (fs + i) % (2 * N_X)) for i in range(1, 2 * N_X)]
    peers += [along_y(i) for i in range(1, N_Y)] + [along_z(i) for i in range(1, N_Z)]
    for peer in peers:
        pl.semaphore_signal(barrier, inc=1, device_id=peer, device_id_type=MESH)
    pl.semaphore_wait(barrier, len(peers))

    class Gather:
        def __init__(self, block, full):
            self.block, self.full, self.copies = block, full, []
            self.xs = [(my_x + i) % N_X for i in range(N_X)]

        def go(self, src, device):
            self.copies.append(send(src, src, device))
            return self.copies[-1]

        def half(self, ref, j):
            return ref.at[half_rows * j:half_rows * (j + 1)]

        def slot(self, step, j):
            return self.half(self.full.at[self.xs[step] * 2 + core], j)

        def start(self):
            mine = self.full.at[fs]
            self.first = [send(self.half(self.block, j), self.half(mine, j), along_x(1 + 2 * j)) for j in range(2)]
            self.second = [send(self.half(self.block, 1 - j), self.half(mine, 1 - j), along_x(1 + 2 * j)) for j in range(2)]
            self.across = send(self.block, mine, partner)
            self.full[fs] = self.block[...]

        def forward(self):
            self.hop = []
            for j, came in ((0, 3), (1, 1)):
                self.first[j].wait_recv()
                self.hop.append(send(self.slot(came, j), self.slot(came, j), along_x(1 + 2 * j)))
                self.go(self.slot(came, j), partner)
            for j, came in ((0, 3), (1, 1)):
                self.second[j].wait_recv()
                self.go(self.slot(came, 1 - j), partner)

        def spread(self):
            for j in range(2):
                self.hop[j].wait_recv()
                self.go(self.slot(2, j), partner)

        def finish(self):
            self.across.wait_recv()
            for copy in self.copies:
                copy.wait_recv()
            for copy in self.copies + self.first + self.second + self.hop + [self.across]:
                copy.wait_send()

    class Ring:
        def __init__(self, along, pos, part, near, full):
            self.along, self.pos, self.part, self.near, self.full = along, pos, part, near, full
            self.far, self.nxt, self.prev = (pos + 2) % 4, (pos + 1) % 4, (pos + 3) % 4

        def start(self):
            self.c = [send(self.part(self.far, 0), self.near(0), self.along(1)), send(self.part(self.far, 1), self.near(1), self.along(3))]

        def direct(self):
            self.c += [send(self.part(self.nxt, 1), self.full(0, 1), self.along(1)), send(self.part(self.prev, 0), self.full(1, 0), self.along(3))]

        def relay(self):
            for way, target in ((0, self.nxt), (1, self.prev)):
                self.c[way].wait_recv()
                self.part(target, way)[...] += self.near(way)[...]
                self.c.append(send(self.part(target, way), self.full(way, way), self.along(1 + 2 * way)))

        def finish(self):
            for copy in self.c[2:]:
                copy.wait_recv()
            self.part(self.pos, None)[...] += self.full(0, None)[...] + self.full(1, None)[...]
            for copy in self.c:
                copy.wait_send()

    def split(start, size, j):
        if j is None:
            return pl.ds(pl.multiple_of(start, 8), size)
        return pl.ds(pl.multiple_of(start + size // 2 * j, 8), size // 2)

    class Reduce:
        def __init__(self, grad, pair_in, out, x_first, lane, width, spare):
            self.out = out
            self.cols = cols = slice(lane, lane + width)
            self.lands = lands = slice(spare, spare + width)
            self.block = grad.at[core, my_x]
            bufs = x_bufs if x_first else y_bufs
            self.z_in = bufs[4]
            near_in = lambda k: (lambda way: bufs[k].at[way, ..., lands])
            full_in = lambda k: (lambda way, j: bufs[k].at[(way,) + (ALL,) * (len(bufs[k].shape) - 3) + (split(0, bufs[k].shape[-2], j), lands)])
            if x_first:
                part_of = lambda c: (lambda i, j: grad.at[c, i, split(0, d_model, j), cols])
                first = (along_x, my_x)
                self.second = Ring(along_y, my_y, lambda i, j: grad.at[core, my_x, split(y_rows * i, y_rows, j), cols], near_in(2), full_in(3))
                self.pair_part = lambda i: pair_in(i, slice(0, d_model), cols)
            else:
                part_of = lambda c: (lambda i, j: grad.at[c, :, split(y_rows * i, y_rows, j), cols])
                first = (along_y, my_y)
                self.second = Ring(along_x, my_x, lambda i, j: grad.at[core, i, split(y_rows * my_y, y_rows, j), cols], near_in(2), full_in(3))
                self.pair_part = lambda i: pair_in(ALL, split(y_rows * i, y_rows, None), cols)
            self.first = Ring(*first, part_of(core), near_in(0), full_in(1))
            self.pair_src = part_of(other)
            self.pair = {}

        def rows_at(self, ref, start, size):
            return ref.at[pl.ds(pl.multiple_of(start, 8), size), self.cols]

        def z_part(self, ref, z):
            return self.rows_at(ref, y_rows * my_y + z_rows * z, z_rows)

        def y_part(self, pos, half=None):
            return self.out.at[split(y_rows * pos, y_rows, half), self.cols]

        def swap(self, name):
            i = getattr(self.first, name)
            self.pair[name] = send(self.pair_src(i, None), self.pair_part(i), partner)

        def merge(self, name):
            i = getattr(self.first, name)
            self.pair[name].wait_recv()
            self.first.part(i, None)[...] += self.pair_part(i)[...]

        def r1(self):
            self.merge('far')
            self.first.start()

        def r1b(self):
            self.merge('nxt')
            self.merge('prev')
            self.first.direct()

        def r2(self):
            self.first.relay()
            self.merge('pos')

        def r3(self):
            for copy in self.pair.values():
                copy.wait_send()
            self.first.finish()
            self.second.start()
            self.second.direct()

        def r4(self):
            self.second.relay()

        def r5(self):
            self.second.finish()
            self.z = [send(self.z_part(self.block, (my_z + i) % N_Z), self.z_in.at[i - 1, :, self.lands], along_z(i)) for i in range(1, N_Z)]

        def r6(self):
            for copy in self.z:
                copy.wait_recv()
            total = self.z_part(self.block, my_z)[...]
            for i in range(1, N_Z):
                total += self.z_in[i - 1, :, self.lands]
            self.z_part(self.out, my_z)[...] = total * scale
            for copy in self.z:
                copy.wait_send()
            self.z = [send(self.z_part(self.out, my_z), self.z_part(self.out, my_z), along_z(i)) for i in range(1, N_Z)]

        def r7(self):
            for copy in self.z:
                copy.wait_recv()
            for copy in self.z:
                copy.wait_send()
            self.c = [send(self.y_part(my_y), self.y_part(my_y), along_y(i)) for i in (1, 3)]

        def r8(self):
            for way, pos in ((0, (my_y + 3) % N_Y), (1, (my_y + 1) % N_Y)):
                self.c[way].wait_recv()
                self.c.append(send(self.y_part(pos, way), self.y_part(pos, way), along_y(1 + 2 * way)))

        def r9(self):
            for copy in self.c[2:]:
                copy.wait_recv()
            for copy in self.c:
                copy.wait_send()

    class Group:
        def __init__(self, parts):
            self.parts = parts

        def r0(self):
            for name in ('far', 'nxt', 'prev', 'pos'):
                for part in self.parts:
                    part.swap(name)

        def __getattr__(self, name):
            def call():
                for part in self.parts:
                    getattr(part, name)()
            return call

    def reduce_all(grad, pair_in, out, plan):
        used = {True: 0, False: 0}
        parts = []
        lane = 0
        for x_first, width in plan:
            parts.append(Reduce(grad, pair_in, out, x_first, lane, width, used[x_first]))
            used[x_first] += width
            lane += width
        return Group(parts)

    class ReduceVec:
        def __init__(self):
            self.rows = vec_out.shape[0] // N_Z

        def part(self, ref, z):
            return ref.at[pl.ds(pl.multiple_of(self.rows * z, 8), self.rows)]

        def swap(self, slots, pos, along):
            return [send(slots.at[pos], slots.at[pos], along(i)) for i in range(1, 4)]

        def total(self, slots, copies):
            for copy in copies:
                copy.wait_recv()
            for copy in copies:
                copy.wait_send()
            return slots[0] + slots[1] + slots[2] + slots[3]

        def r1(self):
            for i in range(d_model // 128):
                vec_pair[0, 32 * i:32 * i + 32] = gv[:, 128 * i:128 * i + 128]
            self.c = [send(vec_pair.at[0], vec_pair.at[1], partner)]

        def r2(self):
            self.c[0].wait_recv()
            vec_x[my_x] = vec_pair[0] + vec_pair[1]
            self.c[0].wait_send()
            self.c = self.swap(vec_x, my_x, along_x)

        def r3(self):
            vec_y[my_y] = self.total(vec_x, self.c)
            self.c = self.swap(vec_y, my_y, along_y)

        def r5(self):
            vec_pair[0] = self.total(vec_y, self.c)
            self.c = [send(self.part(vec_pair.at[0], (my_z + i) % N_Z), vec_z.at[i - 1], along_z(i)) for i in range(1, N_Z)]

        def r6(self):
            for copy in self.c:
                copy.wait_recv()
            total = self.part(vec_pair.at[0], my_z)[...]
            for i in range(1, N_Z):
                total += vec_z[i - 1]
            self.part(vec_out, my_z)[...] = total * scale
            for copy in self.c:
                copy.wait_send()
            self.c = [send(self.part(vec_out, my_z), self.part(vec_out, my_z), along_z(i)) for i in range(1, N_Z)]

        def r7(self):
            for copy in self.c:
                copy.wait_recv()
            for copy in self.c:
                copy.wait_send()

    attn_gather, ffn_gather = Gather(attn_w, aw), Gather(ffn_w, fw)
    vec_copies = [send(vec_w, vec_all.at[fs], (dp, (fs + i) % (2 * N_X))) for i in range(1, 2 * N_X)]
    attn_gather.start()
    vec_all[fs] = vec_w[...]
    attn_gather.forward()
    ffn_gather.start()
    attn_gather.spread()
    for copy in vec_copies:
        copy.wait_recv()
    for copy in vec_copies:
        copy.wait_send()
    pair_rows = 19
    for i in range(N_X * pair_rows):
        p, r = i // pair_rows, i % pair_rows
        if r < 9:
            row = vec_all[2 * p, r:r + 1, :]
        elif r == 9:
            row = vec_all[2 * p, 9:10, :] + vec_all[2 * p + 1, 0:1, :]
        else:
            row = vec_all[2 * p + 1, r - 9:r - 8, :]
        vec[i // 4:i // 4 + 1, i % 4 * 128:i % 4 * 128 + 128] = row
    attn_gather.finish()
    for load in loads:
        load.wait()

    ffn_reduce = reduce_all(gf, lambda i, r, c: ga.at[0, i, r, c], ffn_out, FFN_PLAN)
    attn_reduce = reduce_all(ga, lambda i, r, c: gp.at[i, r, c], attn_out, ATTN_PLAN)
    vec_reduce = ReduceVec()

    def rows(r):
        return pl.ds(pl.multiple_of(r * ROWS, ROWS), ROWS)

    def bias(i):
        return vec[i:i + 1, :]

    def add_vec(i, val):
        gv[pl.ds(i, 1), :] += jnp.sum(val, axis=0, keepdims=True)

    def norm(res):
        cen = res - jnp.mean(res, axis=-1, keepdims=True)
        inv = lax.rsqrt(jnp.mean(cen * cen, axis=-1, keepdims=True) + LN_EPS)
        return cen * inv, inv

    def norm_grad(d_out, normed, inv, slot):
        add_vec(slot, d_out * normed)
        add_vec(slot + 1, d_out)
        d_norm = d_out * bias(slot)
        return inv * (d_norm - jnp.mean(d_norm, axis=-1, keepdims=True) - normed * jnp.mean(d_norm * normed, axis=-1, keepdims=True))

    gv[...] = jnp.zeros_like(gv)

    def proj_self(r, _):
        s = rows(r)
        xr = x[s, :]
        er = enc[s, :]
        q[s, :] = ((mm(xr, aw[0]) + bias(0)) * 0.125).astype(BF)
        k[s, :] = (mm(xr, aw[1]) + bias(1)).astype(BF)
        v[s, :] = (mm(xr, aw[2]) + bias(2)).astype(BF)
        kc[s, :] = (mm(er, aw[5]) + bias(5)).astype(BF)
        vc[s, :] = (mm(er, aw[6]) + bias(6)).astype(BF)
        return 0

    lax.fori_loop(0, n_chunks, proj_self, 0)

    low_half = lax.broadcasted_iota(jnp.int32, (n_tgt, 128), 1) < 64

    def half(val, j):
        return jnp.where(low_half if j == 0 else ~low_half, val, jnp.zeros_like(val))

    def both(val):
        return jnp.concatenate([half(val, 0), half(val, 1)], axis=0)

    def key_mask(b, causal):
        key_pos = lax.broadcasted_iota(jnp.int32, (n_tgt, n_src), 1)
        if causal:
            return (key_pos <= lax.broadcasted_iota(jnp.int32, (n_tgt, n_src), 0)) & (key_pos < tgt_lens[b])
        return key_pos < src_lens[b]

    def prob(qm, k2, mask):
        sc = jnp.where(mask, mm_nt(qm, k2), MASK_FILL)
        e = jnp.exp(sc - jnp.max(sc, axis=-1, keepdims=True))
        return e * (1.0 / jnp.sum(e, axis=-1, keepdims=True))

    def attn(q, k, v, o, causal):
        def step(i, _):
            b = i // n_pairs
            hp = i % n_pairs
            s = pl.ds(pl.multiple_of(b * n_tgt, n_tgt), n_tgt)
            c = pl.ds(pl.multiple_of(hp * 128, 128), 128)
            q2, k2, v2 = q[s, c], k[s, c], v[s, c]
            mask = key_mask(b, causal)
            mask = jnp.concatenate([mask, mask], axis=0)
            outs = mm(prob(both(q2), k2, mask).astype(BF), v2)
            o[s, c] = jnp.where(low_half, outs[:n_tgt], outs[n_tgt:]).astype(BF)
            return 0
        lax.fori_loop(0, n_batch * n_pairs, step, 0)

    def attn_grad(q, k, v, do, causal, begin, end):
        def step(i, _):
            b = i // n_pairs
            hp = i % n_pairs
            s = pl.ds(pl.multiple_of(b * n_tgt, n_tgt), n_tgt)
            c = pl.ds(pl.multiple_of(hp * 128, 128), 128)
            q2, k2, v2, do2 = q[s, c], k[s, c], v[s, c], do[s, c]
            mask = key_mask(b, causal)
            qt, dot = q2.T, do2.T
            p = prob(both(q2), k2, jnp.concatenate([mask, mask], axis=0))
            dp = mm_nt(both(do2), v2)
            ds = (p * (dp - jnp.sum(p * dp, axis=-1, keepdims=True))).astype(BF)
            pb = p.astype(BF)
            dq = mm(ds, k2)
            dvt = [mm(dot[64 * j:64 * j + 64], pb[n_tgt * j:n_tgt * (j + 1)]) for j in range(2)]
            dkt = [mm(qt[64 * j:64 * j + 64], ds[n_tgt * j:n_tgt * (j + 1)]) for j in range(2)]
            q[s, c] = (jnp.where(low_half, dq[:n_tgt], dq[n_tgt:]) * 0.125).astype(BF)
            k[s, c] = jnp.concatenate(dkt, axis=0).astype(BF).T
            v[s, c] = jnp.concatenate(dvt, axis=0).astype(BF).T
            return 0
        steps = n_batch * n_pairs
        lax.fori_loop(begin * steps // 4, end * steps // 4, step, 0)

    attn(q, k, v, o, True)
    ffn_gather.forward()

    def post_self(r, _):
        s = rows(r)
        n1[s, :], i1[s, :] = norm(x[s, :].astype(F32) + mm(o[s, :], aw[3]) + bias(3))
        h = (n1[s, :] * bias(9) + bias(10)).astype(BF)
        h1[s, :] = h
        qc[s, :] = ((mm(h, aw[4]) + bias(4)) * 0.125).astype(BF)
        return 0

    lax.fori_loop(0, n_chunks, post_self, 0)
    attn(qc, kc, vc, oc, False)
    ffn_gather.spread()
    ffn_gather.finish()

    def ffn(r, _):
        s = rows(r)
        n2[s, :], i2[s, :] = norm(h1[s, :].astype(F32) + mm(oc[s, :], aw[7]) + bias(7))
        h = (n2[s, :] * bias(11) + bias(12)).astype(BF)
        h2[s, :] = h
        acc[s, :] = h.astype(F32) + bias(8)

        def up(f, _):
            u = mm_nt(h2[s, :], fw[f]) + vec[pl.ds(15 + f, 1), :]
            cdf = 0.5 * (1.0 + lax.erf(u * 0.7071067811865476))
            g_out = (u * cdf).astype(BF)
            g[f, s, :] = g_out
            gp[f, s, :] = cdf + u * (0.3989422804014327 * jnp.exp(-0.5 * u * u))
            acc[s, :] += mm(g_out, fw[n_ffn + f])
            return 0

        lax.fori_loop(0, n_ffn, up, 0)
        normed, inv = norm(acc[s, :])
        y[s, :] = (normed * bias(13) + bias(14)).astype(BF)
        d3 = norm_grad(dy[s, :].astype(F32), normed, inv, 13)
        add_vec(8, d3)
        dres[s, :] = d3
        dresb[s, :] = d3.astype(BF)
        return 0

    lax.fori_loop(0, n_chunks, ffn, 0)
    stores[0].start()

    def ffn_grad(f, _):
        gf[(n_ffn + f) % 2, (n_ffn + f) // 2] = mm_tn(g[f], dresb[...])

        def up_grad(r, _):
            s = rows(r)
            d_up = mm_nt(dresb[s, :], fw[n_ffn + f]) * gp[f, s, :]
            add_vec(15 + f, d_up)
            d_up = d_up.astype(BF)
            g[f, s, :] = d_up
            dres[s, :] += mm(d_up, fw[f])
            return 0

        lax.fori_loop(0, n_chunks, up_grad, 0)
        gf[f % 2, f // 2] = mm_tn(g[f], h2[...])
        return 0

    lax.fori_loop(0, n_ffn, ffn_grad, 0)
    ffn_reduce.r0()

    def norm2_grad(r, _):
        s = rows(r)
        d2 = norm_grad(dres[s, :], n2[s, :], i2[s, :], 11)
        add_vec(7, d2)
        dres[s, :] = d2
        d2 = d2.astype(BF)
        dresb[s, :] = d2
        h2[s, :] = mm_nt(d2, aw[7]).astype(BF)
        return 0

    lax.fori_loop(0, n_chunks, norm2_grad, 0)
    ga[1, 3] = mm_tn(oc[...], dresb[...])
    ffn_reduce.r1()
    ffn_reduce.r1b()
    attn_grad(qc, kc, vc, h2, False, 0, 2)
    ffn_reduce.r2()
    attn_grad(qc, kc, vc, h2, False, 2, 4)
    ga[0, 2] = mm_tn(h1[...], qc[...])
    ga[1, 2] = mm_tn(enc[...], kc[...])
    ga[0, 3] = mm_tn(enc[...], vc[...])

    def norm1_grad(r, _):
        s = rows(r)
        d1 = norm_grad(dres[s, :] + mm_nt(qc[s, :], aw[4]), n1[s, :], i1[s, :], 9)
        add_vec(3, d1)
        dres[s, :] = d1
        d1 = d1.astype(BF)
        dresb[s, :] = d1
        h2[s, :] = mm_nt(d1, aw[3]).astype(BF)
        return 0

    lax.fori_loop(0, n_chunks, norm1_grad, 0)
    ga[1, 1] = mm_tn(o[...], dresb[...])
    attn_grad(q, k, v, h2, True, 0, 2)
    ffn_reduce.r3()
    attn_grad(q, k, v, h2, True, 2, 3)
    ffn_reduce.r4()
    attn_grad(q, k, v, h2, True, 3, 4)
    ffn_reduce.r5()
    ga[0, 0] = mm_tn(x[...], q[...])
    ga[1, 0] = mm_tn(x[...], k[...])
    ga[0, 1] = mm_tn(x[...], v[...])

    attn_reduce.r0()
    ffn_reduce.r6()
    attn_reduce.r1()
    attn_reduce.r1b()

    def last(r, _):
        s = rows(r)
        add_vec(4, qc[s, :].astype(F32))
        add_vec(5, kc[s, :].astype(F32))
        add_vec(6, vc[s, :].astype(F32))
        denc[s, :] = (mm_nt(kc[s, :], aw[5]) + mm_nt(vc[s, :], aw[6])).astype(BF)
        add_vec(0, q[s, :].astype(F32))
        add_vec(1, k[s, :].astype(F32))
        add_vec(2, v[s, :].astype(F32))
        dx[s, :] = (dres[s, :] + mm_nt(q[s, :], aw[0]) + mm_nt(k[s, :], aw[1]) + mm_nt(v[s, :], aw[2])).astype(BF)
        return 0

    lax.fori_loop(0, n_chunks, last, 0)
    stores[1].start()
    stores[2].start()
    vec_reduce.r1()
    ffn_reduce.r7()
    attn_reduce.r2()
    vec_reduce.r2()
    attn_reduce.r3()
    vec_reduce.r3()
    ffn_reduce.r8()
    attn_reduce.r4()
    vec_reduce.r5()
    attn_reduce.r5()
    attn_reduce.r6()
    vec_reduce.r6()
    attn_reduce.r7()
    vec_reduce.r7()
    ffn_reduce.r9()
    attn_reduce.r8()
    attn_reduce.r9()
    for store in stores:
        store.wait()
    assert sem_count[0] <= send_sems.shape[0]


def copy_out(*refs):
    for src, dst in zip(refs[:5], refs[5:]):
        dst[...] = src[...]


def solution(mesh):
    n_fsdp = mesh.shape['fsdp']
    n_dp = mesh.shape['dp']
    batch_axes = ('dp', 'fsdp')
    act_spec = P(batch_axes, None, None)
    len_spec = P(batch_axes)
    row_spec = P('fsdp', None)
    vec_spec = P('fsdp')

    def device_step(dec_in, enc_out, src_lens, tgt_lens, y_cot, attn_w, ffn_w, vec_params):
        n_batch, n_tgt, d = dec_in.shape
        n_src = enc_out.shape[1]
        n_tok = n_batch * n_tgt
        n_vec = vec_params.shape[0]
        ffn_dim = n_fsdp * ffn_w.shape[0] // 2
        n_ffn = ffn_dim // d
        scale = 1.0 / (n_tok * n_fsdp * n_dp)
        fs = lax.axis_index('fsdp')
        vec_f = vec_params.astype(F32)
        vec_w = jnp.where(fs % 2 == 0, jnp.pad(vec_f, (0, 2048 - n_vec)), jnp.pad(vec_f, (64, 2048 - 64 - n_vec))).reshape(16, 128)
        vm = pl.BlockSpec(memory_space=pltpu.VMEM)
        hbm = pl.BlockSpec(memory_space=pl.ANY)
        sm = pl.BlockSpec(memory_space=pltpu.SMEM)
        act = jax.ShapeDtypeStruct((n_tok, d), BF)
        block = jax.ShapeDtypeStruct((d, d), F32)
        half = d // 2
        buf = lambda *shape: pltpu.VMEM(shape, F32)
        tok = lambda dt: pltpu.VMEM((n_tok, d), dt)
        col = pltpu.VMEM((n_tok, 1), F32)
        weights = pltpu.VMEM((n_fsdp, d, d), BF)
        y, dx, denc, ga, gf, gv = pl.pallas_call(
            functools.partial(layer_kernel, n_batch, n_tgt, n_src, d, ffn_dim, scale),
            out_shape=(act, act, act, block, block, jax.ShapeDtypeStruct((128, 128), F32)),
            in_specs=[sm, sm] + [hbm] * 3 + [vm] * 3,
            out_specs=(hbm,) * 3 + (vm,) * 3,
            scratch_shapes=[tok(BF)] * 5 + [pltpu.SemaphoreType.DMA((6,)), weights, weights, buf(2, N_X, d, d), buf(2, N_X, d, d), buf(32, d), buf(24, d), buf(n_fsdp, 16, 128)]
            + [tok(BF)] * 4 + [tok(BF), tok(F32), col] + [tok(BF)] * 4 + [tok(F32), col, tok(BF)]
            + [buf(n_ffn, n_tok, d), pltpu.VMEM((n_ffn, n_tok, d), BF), tok(F32), tok(BF)]
            + [buf(2, d // 2, half), buf(2, d, half), buf(2, 64, half), buf(2, 128, half), buf(7, 16, half)]
            + [buf(2, N_X, 64, half), buf(2, N_X, 128, half), buf(2, 64, half), buf(2, 128, half), buf(7, 16, half)]
            + [buf(2, 128, 128), buf(4, 128, 128), buf(4, 128, 128), buf(7, 16, 128)]
            + [pltpu.SemaphoreType.DMA((260,)), pltpu.SemaphoreType.DMA((260,))],
            compiler_params=pltpu.CompilerParams(vmem_limit_bytes=67043328, collective_id=0, has_side_effects=True),
            cost_estimate=pl.CostEstimate(flops=24 * 10**9, bytes_accessed=30 * 2**20, transcendentals=0),
            name='layer',
        )(src_lens, tgt_lens, dec_in.reshape(n_tok, d), enc_out.reshape(n_tok, d), y_cot.reshape(n_tok, d), attn_w, ffn_w, vec_w)
        n_steps = 4
        tiles = [pl.BlockSpec((arr.shape[0] // n_steps, d), lambda i: (i, 0)) for arr in (y, dx, denc, ga, gf)]
        y, dx, denc, ga, gf = pl.pallas_call(
            copy_out,
            grid=(n_steps,),
            out_shape=tuple(jax.ShapeDtypeStruct(arr.shape, arr.dtype) for arr in (y, dx, denc, ga, gf)),
            in_specs=tiles,
            out_specs=tuple(tiles),
            compiler_params=pltpu.CompilerParams(vmem_limit_bytes=67043328),
            name='out',
        )(y, dx, denc, ga, gf)
        gv = gv.reshape(d // 128, 32, 128).transpose(1, 0, 2).reshape(-1)
        gv = lax.dynamic_slice_in_dim(gv, fs * n_vec, n_vec)
        return y.reshape(dec_in.shape), dx.reshape(dec_in.shape), denc.reshape(enc_out.shape), ga, gf, gv

    return jax.shard_map(device_step, mesh=mesh, in_specs=(act_spec, act_spec, len_spec, len_spec, act_spec, row_spec, row_spec, vec_spec), out_specs=(act_spec, act_spec, act_spec, row_spec, row_spec, vec_spec), check_vma=False)
```
